256 devices in a mesh: dp: 16 (over z_hi, x), row: 2 (over z_lo), col: 8 (over y, core).
Axes of the slice: x: 4, y: 4, z: 8 (z_hi: 4, z_lo: 2; z = z_hi * 2 + z_lo), core: 2. Of those that a mesh axis runs over, the one named last changes fastest.
Arguments:
- activations: bfloat16 [16384, 2048], P('dp', ('row', 'col')), may hold values from -0.08984375 to 0.08984375
- gate_input: bfloat16 [16384, 5120], P('dp', ('row', 'col')), may hold values from -6 to 6
- up_input: bfloat16 [16384, 5120], P('dp', ('row', 'col')), may hold values from -6 to 6
- hidden_grad: bfloat16 [16384, 5120], P('dp', ('row', 'col')), may hold values from -6 to 6
- weight_gate: bfloat16 [2048, 5120], P(None, ('row', 'col')), may hold values from -0.125 to 0.125
- weight_up: bfloat16 [2048, 5120], P(None, ('row', 'col')), may hold values from -0.125 to 0.125
Outputs:
- input_grad: float32 [16384, 2048], P('dp', ('row', 'col'))
- gate_weight_grad: float32 [2048, 5120], P(None, ('row', 'col'))
- up_weight_grad: float32 [2048, 5120], P(None, ('row', 'col'))
The draws below stay inside these ranges and needn't reach their ends.
All inputs are finite; a program needn't handle non-finite values.
Results may differ from the reference program's by a relative error of at most 0.0029.
Values may be sent and summed in bfloat16 or wider, within the bound.
A program may use at most 128 MiB of HBM per device.

```python
import jax
import jax.numpy as jnp
from jax import lax

D = 2048
FF = 5120
TOKENS = 16384


def levels(own_key, shape, cuts, smallest, largest):
    def one(position, parts):
        draws = jax.random.uniform(jax.random.fold_in(jax.random.fold_in(own_key, 6), position), (parts,), jnp.float32, smallest / len(cuts), largest / len(cuts))
        return jnp.repeat(jnp.exp(draws), shape[position] // parts).reshape((-1,) + (1,) * (len(shape) - position - 1))

    loudness = one(*cuts[0])
    for cut in cuts[1:]:
        loudness = loudness * one(*cut)
    return loudness


def bell_draw(own_key, shape, spread, most, cuts=(), dtype=jnp.bfloat16):
    entries = spread * jax.random.normal(own_key, shape, jnp.float32)
    if cuts:
        entries = entries * levels(own_key, shape, cuts, -0.22, 0.18)
    return jnp.clip(entries, -most, most).astype(dtype)


def setup_inputs(seed: int = 0) -> dict:
    streams_of = jax.random.split(jax.random.key(seed), 7)
    activations = bell_draw(streams_of[0], (TOKENS, D), 0.015, 0.08984375, ((0, 16), (1, 16)))
    gate_input = bell_draw(streams_of[1], (TOKENS, FF), 1.0, 6.0, ((0, 16), (1, 16)))
    up_input = bell_draw(streams_of[2], (TOKENS, FF), 1.0, 6.0, ((0, 16), (1, 16)))
    hidden_grad = bell_draw(streams_of[3], (TOKENS, FF), 1.0, 6.0, ((0, 16), (1, 16)))
    weight_gate = bell_draw(streams_of[4], (D, FF), D ** -0.5, 0.125, ((1, 16),))
    weight_up = bell_draw(streams_of[5], (D, FF), D ** -0.5, 0.125, ((1, 16),))
    return dict(activations=activations, gate_input=gate_input, up_input=up_input, hidden_grad=hidden_grad, weight_gate=weight_gate, weight_up=weight_up)


ROOT_TWO_PI = 0.7978845608028654
CUBIC = 0.044715


def reference(activations, gate_input, up_input, hidden_grad, weight_gate, weight_up):
    gate_pre = gate_input.astype(jnp.float32)
    up_pre = up_input.astype(jnp.float32)
    grad_hidden = hidden_grad.astype(jnp.float32)
    tanh_part = jnp.tanh(ROOT_TWO_PI * (gate_pre + CUBIC * gate_pre * gate_pre * gate_pre))
    gelu_value = 0.5 * gate_pre * (1.0 + tanh_part)
    gelu_slope = 0.5 * (1.0 + tanh_part) + 0.5 * gate_pre * (1.0 - tanh_part * tanh_part) * ROOT_TWO_PI * (1.0 + 3.0 * CUBIC * gate_pre * gate_pre)
    gate_grad = (grad_hidden * up_pre * gelu_slope).astype(jnp.bfloat16)
    up_grad = (grad_hidden * gelu_value).astype(jnp.bfloat16)
    dims_feature = (((1,), (1,)), ((), ()))
    dims_tokens = (((0,), (0,)), ((), ()))
    input_grad = lax.dot_general(gate_grad, weight_gate, dims_feature, preferred_element_type=jnp.float32)
    input_grad = input_grad + lax.dot_general(up_grad, weight_up, dims_feature, preferred_element_type=jnp.float32)
    gate_weight_grad = lax.dot_general(activations, gate_grad, dims_tokens, preferred_element_type=jnp.float32)
    up_weight_grad = lax.dot_general(activations, up_grad, dims_tokens, preferred_element_type=jnp.float32)
    return input_grad.astype(jnp.float32), gate_weight_grad, up_weight_grad
```

```python
import functools

import jax
import jax.numpy as jnp
from jax import lax
from jax.experimental import pallas as pl
from jax.experimental.pallas import tpu as pltpu
from jax.sharding import PartitionSpec as P

ROOT_TWO_PI = 0.7978845608028654
CUBIC = 0.044715
MESH = pl.DeviceIdType.MESH
F32, BF16 = jnp.float32, jnp.bfloat16

TOK = 1024
HID = 320
WIDE = 2 * HID
COLS = 128
D = 2048
CHUNKS = 8
CH = D // CHUNKS
XR = CH // 4
ZR = XR // 4
NT = (((1,), (1,)), ((), ()))


def geglu_grads(gate_input, up_input, hidden_grad):
    gate_pre = gate_input.astype(F32)
    up_pre = up_input.astype(F32)
    grad_hidden = hidden_grad.astype(F32)
    tanh_part = jnp.tanh(ROOT_TWO_PI * (gate_pre + CUBIC * gate_pre * gate_pre * gate_pre))
    gelu_value = 0.5 * gate_pre * (1.0 + tanh_part)
    gelu_slope = 0.5 * (1.0 + tanh_part) + 0.5 * gate_pre * (
        1.0 - tanh_part * tanh_part
    ) * ROOT_TWO_PI * (1.0 + 3.0 * CUBIC * gate_pre * gate_pre)
    return (grad_hidden * up_pre * gelu_slope).astype(BF16), (grad_hidden * gelu_value).astype(BF16)


def store_packed(ref, rows, first, second):
    ref[rows, 0:256] = first[:, 0:256]
    ref[rows, 256:512] = second[:, 0:256]
    ref[rows, 512:640] = jnp.concatenate([first[:, 256:320], second[:, 256:320]], axis=1)


def kernel(
    act_h, gate_h, up_h, hid_h, wg_h, wu_h,
    w_out, own_out, last_out,
    act_v, gate_v, up_v, hid_v, wg_v, wu_v, wp, gp, ag,
    part, xs, xr, x3, qs, q1, zr, z3, z3r,
    pkeep, bs, br, ykeep, ys, yr, y3, tz,
    in_sem, ag_recv, ag_send, c_recv, c_send, b_recv, b_send, y_recv, y_send, t_recv, t_send,
):
    dp, row, col = lax.axis_index("dp"), lax.axis_index("row"), lax.axis_index("col")
    zh, x = dp // 4, lax.rem(dp, 4)
    y, core = col // 2, lax.rem(col, 2)
    s = 2 * core - 1

    def at(base, step):
        return lax.rem(base + step + 4, 4)

    def dev(dx=0, dzh=0, dy=0, flip_row=False, flip_core=False):
        return (
            at(zh, dzh) * 4 + at(x, dx),
            1 - row if flip_row else row,
            at(y, dy) * 2 + (1 - core if flip_core else core),
        )

    x_up, x_down = dev(dx=s), dev(dx=-s)
    z_up, z_down = dev(dzh=s), dev(dzh=-s)
    y_up, y_down = dev(dy=s), dev(dy=-s)
    pair, mate = dev(flip_row=True), dev(flip_core=True)

    loads = []
    for n, (src, dst) in enumerate(
        ((act_h, act_v), (gate_h, gate_v), (up_h, up_v), (hid_h, hid_v), (wg_h, wg_v), (wu_h, wu_v))
    ):
        loads.append(pltpu.make_async_copy(src, dst, in_sem.at[n]))
        loads[-1].start()

    barrier = pltpu.get_barrier_semaphore()
    for other in (x_up, x_down, z_up, z_down, y_up, y_down, pair, mate):
        pl.semaphore_signal(barrier, inc=1, device_id=other, device_id_type=MESH)

    sent = []

    def send(src, dst, send_sem, recv_sem, to):
        copy = pltpu.make_async_remote_copy(
            src_ref=src, dst_ref=dst, send_sem=send_sem, recv_sem=recv_sem,
            device_id=to, device_id_type=MESH,
        )
        copy.start()
        sent.append(copy)

    def arrived(dst, recv_sem, send_sem):
        pltpu.make_async_remote_copy(
            src_ref=dst, dst_ref=dst, send_sem=send_sem, recv_sem=recv_sem,
            device_id=mate, device_id_type=MESH,
        ).wait_recv()

    def place(other_row, dy, other_core=False):
        return (1 - row if other_row else row) * 8 + at(y, dy) * 2 + (1 - core if other_core else core)

    n_ag = [0]

    def ag_give(slot, to):
        send(ag.at[slot], ag.at[slot], ag_send.at[n_ag[0]], ag_recv.at[slot], to)
        n_ag[0] += 1

    def ag_take(slot):
        arrived(ag.at[slot], ag_recv.at[slot], ag_send.at[0])

    own = place(False, 0)
    loads[0].wait()
    ag[own] = act_v[...].T
    pl.semaphore_wait(barrier, 8)
    for to in (pair, y_up, y_down, mate):
        ag_give(own, to)

    for load in loads[1:4]:
        load.wait()

    def gate_rows(i, carry):
        rows = pl.ds(pl.multiple_of(i * 64, 64), 64)
        store_packed(gp, rows, *geglu_grads(gate_v[rows, :], up_v[rows, :], hid_v[rows, :]))
        return carry

    lax.fori_loop(0, TOK // 64, gate_rows, 0)

    order = ((False, 0), (True, 0), (False, -s), (False, s), (True, -s), (True, s), (False, 2), (True, 2))

    def base_row(k):
        other_row, dy = order[k]
        return pl.multiple_of(((1 - row if other_row else row) * 8 + at(y, dy) * 2) * COLS, CH)

    def c_give(k, n, src, dst, to):
        send(src, dst, c_send.at[k, n], c_recv.at[k, n], to)

    def c_take(k, n, dst):
        arrived(dst, c_recv.at[k, n], c_send.at[k, n])

    def x_rows(place_x):
        return pl.ds(pl.multiple_of(place_x * XR, XR), XR)

    def c0(k):
        other_row, dy = order[k]
        ag_take(place(other_row, dy, True))
        first = pl.multiple_of(place(other_row, dy) - core, 2)
        lhs = ag[pl.ds(first, 2)].reshape(CH, TOK)
        part[k] = jnp.dot(lhs, gp[...], preferred_element_type=F32)
        xs[k, 0] = part[k, x_rows(at(x, 2)), :].astype(BF16)
        c_give(k, 0, xs.at[k, 0], xr.at[k, 0], x_up)
        xs[k, 1] = part[k, x_rows(at(x, -s)), :].astype(BF16)
        c_give(k, 1, xs.at[k, 1], xr.at[k, 1], x_down)

    def c1(k):
        c_take(k, 0, xr.at[k, 0])
        x3[k] = (part[k, x_rows(at(x, s)), :] + xr[k, 0].astype(F32)).astype(BF16)
        c_give(k, 2, x3.at[k], xr.at[k, 2], x_up)

    def c2(k):
        c_take(k, 1, xr.at[k, 1])
        c_take(k, 2, xr.at[k, 2])
        q1[k] = part[k, x_rows(x), :] + xr[k, 1].astype(F32) + xr[k, 2].astype(F32)
        qs[k, 0] = q1[k, z_rows(at(zh, 2)), :].astype(BF16)
        c_give(k, 3, qs.at[k, 0], zr.at[k, 0], z_up)
        qs[k, 1] = q1[k, z_rows(at(zh, -s)), :].astype(BF16)
        c_give(k, 4, qs.at[k, 1], zr.at[k, 1], z_down)

    def z_rows(place_z):
        return pl.ds(pl.multiple_of(place_z * ZR, ZR), ZR)

    def c3(k):
        c_take(k, 3, zr.at[k, 0])
        z3[k] = q1[k, z_rows(at(zh, s)), :] + zr[k, 0].astype(F32)
        c_give(k, 5, z3.at[k], z3r.at[k], z_up)

    def out_x(k, place_x):
        return w_out.at[pl.ds(pl.multiple_of(base_row(k) + place_x * XR, XR), XR), :]

    def out_z(k, place_z):
        return w_out.at[pl.ds(pl.multiple_of(base_row(k) + x * XR + place_z * ZR, ZR), ZR), :]

    def c4(k):
        c_take(k, 4, zr.at[k, 1])
        c_take(k, 5, z3r.at[k])
        total = q1[k, z_rows(zh), :] + zr[k, 1].astype(F32) + z3r[k]
        mine = out_z(k, zh)
        mine[...] = total.astype(BF16)
        c_give(k, 6, mine, mine, z_up)
        c_give(k, 7, mine, mine, z_down)

    def c5(k):
        got = out_z(k, at(zh, -s))
        c_take(k, 6, got)
        c_give(k, 8, got, got, z_up)

    def c6(k):
        c_take(k, 7, out_z(k, at(zh, s)))
        c_take(k, 8, out_z(k, at(zh, 2)))
        mine = out_x(k, x)
        c_give(k, 9, mine, mine, x_up)
        c_give(k, 10, mine, mine, x_down)

    def c7(k):
        got = out_x(k, at(x, -s))
        c_take(k, 9, got)
        c_give(k, 11, got, got, x_up)

    def c8(k):
        c_take(k, 10, out_x(k, at(x, s)))
        c_take(k, 11, out_x(k, at(x, 2)))

    def ag_pair():
        slot = place(True, 0)
        ag_take(slot)
        for to in (y_up, y_down, mate):
            ag_give(slot, to)

    def ag_near(other_row):
        slot = place(other_row, -s)
        ag_take(slot)
        ag_give(slot, y_up)
        ag_give(slot, mate)
        slot = place(other_row, s)
        ag_take(slot)
        ag_give(slot, mate)

    def ag_far(other_row):
        slot = place(other_row, 2)
        ag_take(slot)
        ag_give(slot, mate)

    def pack_weights():
        loads[4].wait()
        loads[5].wait()

        def step(i, carry):
            rows = pl.ds(pl.multiple_of(i * 128, 128), 128)
            store_packed(wp, rows, wg_v[rows, :], wu_v[rows, :])
            return carry

        lax.fori_loop(0, D // 128, step, 0)

    def b0(i):
        first = ((i // 4) * 8 + at(y, i % 4) * 2) * COLS
        mine = wp[pl.ds(pl.multiple_of(first + core * COLS, COLS), COLS), :]
        others = wp[pl.ds(pl.multiple_of(first + (1 - core) * COLS, COLS), COLS), :]
        both = jnp.concatenate([mine, others], axis=0)

        def step(r, carry):
            rows = pl.ds(pl.multiple_of(r * 256, 256), 256)
            sums = lax.dot_general(gp[rows, :], both, NT, preferred_element_type=F32)
            pkeep[i, rows, :] = sums[:, 0:COLS]
            bs[i, rows, :] = sums[:, COLS : 2 * COLS].astype(BF16)
            return carry

        lax.fori_loop(0, TOK // 256, step, 0)
        send(bs.at[i], br.at[i], b_send.at[i], b_recv.at[i], mate)

    def b1(r):
        for i in range(4 * r, 4 * r + 4):
            arrived(br.at[i], b_recv.at[i], b_send.at[i])

        def pair_sum(off):
            i = 4 * r + at(0, off)
            return pkeep[i] + br[i].astype(F32)

        ys[r, 0] = pair_sum(2).astype(BF16)
        send(ys.at[r, 0], yr.at[r, 0], y_send.at[r, 0], y_recv.at[r, 0], y_up)
        ys[r, 1] = pair_sum(-s).astype(BF16)
        send(ys.at[r, 1], yr.at[r, 1], y_send.at[r, 1], y_recv.at[r, 1], y_down)
        ykeep[r, 0] = pair_sum(s)
        ykeep[r, 1] = pair_sum(0)

    def b2(r):
        arrived(yr.at[r, 0], y_recv.at[r, 0], y_send.at[r, 0])
        y3[r] = (ykeep[r, 0] + yr[r, 0].astype(F32)).astype(BF16)
        send(y3.at[r], yr.at[r, 2], y_send.at[r, 2], y_recv.at[r, 2], y_up)

    def b3():
        for r in range(2):
            for n in (1, 2):
                arrived(yr.at[r, n], y_recv.at[r, n], y_send.at[r, n])

        def total(r):
            return ykeep[r, 1] + yr[r, 1].astype(F32) + yr[r, 2].astype(F32)

        tz[...] = total(1 - row).astype(BF16)
        send(tz, last_out, t_send, t_recv, pair)
        own_out[...] = total(row)

    def b4():
        arrived(last_out, t_recv, t_send)

    extra = {
        0: (pack_weights, lambda: b0(0), lambda: b0(1), lambda: b0(2), lambda: b0(3), ag_pair),
        1: (lambda: ag_near(False), lambda: b0(4), lambda: b0(5)),
        2: (lambda: b0(6), lambda: b0(7)),
        3: (),
        4: (lambda: ag_near(True),),
        5: (lambda: b1(0), lambda: b1(1)),
        6: (lambda: ag_far(False),),
        7: (lambda: ag_far(True),),
        8: (lambda: b2(0), lambda: b2(1)),
        12: (b3,),
    }
    stages = (c0, c1, c2, c3, c4, c5, c6, c7, c8)
    before = {2, 4, 6, 7}
    for t in range(CHUNKS + len(stages) - 1):
        if t in before:
            for f in extra.get(t, ()):
                f()
        for n in range(len(stages) - 1, -1, -1):
            if 0 <= t - n < CHUNKS:
                stages[n](t - n)
        if t not in before:
            for f in extra.get(t, ()):
                f()
    b4()
    for copy in sent:
        copy.wait_send()


def exchange(*args):
    vmem = pltpu.VMEM
    dma = pltpu.SemaphoreType.DMA
    return pl.pallas_call(
        kernel,
        name="exchange",
        out_shape=(
            jax.ShapeDtypeStruct((D, WIDE), BF16),
            jax.ShapeDtypeStruct((TOK, COLS), F32),
            jax.ShapeDtypeStruct((TOK, COLS), BF16),
        ),
        in_specs=[pl.BlockSpec(memory_space=pl.ANY)] * 6,
        out_specs=[pl.BlockSpec(memory_space=pltpu.VMEM)] * 3,
        scratch_shapes=[
            vmem((TOK, COLS), BF16), vmem((TOK, HID), BF16), vmem((TOK, HID), BF16), vmem((TOK, HID), BF16),
            vmem((D, HID), BF16), vmem((D, HID), BF16), vmem((D, WIDE), BF16), vmem((TOK, WIDE), BF16),
            vmem((16, COLS, TOK), BF16),
            vmem((CHUNKS, CH, WIDE), F32), vmem((CHUNKS, 2, XR, WIDE), BF16), vmem((CHUNKS, 3, XR, WIDE), BF16),
            vmem((CHUNKS, XR, WIDE), BF16), vmem((CHUNKS, 2, ZR, WIDE), BF16), vmem((CHUNKS, XR, WIDE), F32),
            vmem((CHUNKS, 2, ZR, WIDE), BF16), vmem((CHUNKS, ZR, WIDE), F32), vmem((CHUNKS, ZR, WIDE), F32),
            vmem((8, TOK, COLS), F32), vmem((8, TOK, COLS), BF16), vmem((8, TOK, COLS), BF16),
            vmem((2, 2, TOK, COLS), F32), vmem((2, 2, TOK, COLS), BF16), vmem((2, 3, TOK, COLS), BF16),
            vmem((2, TOK, COLS), BF16), vmem((TOK, COLS), BF16),
            dma((6,)), dma((16,)), dma((16,)), dma((CHUNKS, 12)), dma((CHUNKS, 12)), dma((8,)), dma((8,)),
            dma((2, 3)), dma((2, 3)), dma, dma,
        ],
        compiler_params=pltpu.CompilerParams(
            collective_id=0, has_side_effects=True, vmem_limit_bytes=63 * 1024 * 1024
        ),
        cost_estimate=pl.CostEstimate(flops=5 * 10**9, bytes_accessed=10**7, transcendentals=0),
    )(*args)


def finish_kernel(w_ref, own_ref, last_ref, x_ref, gate_ref, up_ref):
    w = w_ref[...].astype(F32)
    gate_ref[:, 0:256] = w[:, 0:256]
    up_ref[:, 0:256] = w[:, 256:512]
    gate_ref[:, 256:320] = w[:, 512:576]
    up_ref[:, 256:320] = w[:, 576:640]
    x_ref[...] = own_ref[...] + last_ref[...].astype(F32)


def finish(w, own, last):
    steps = 8
    return pl.pallas_call(
        finish_kernel,
        name="finish",
        grid=(steps,),
        out_shape=(
            jax.ShapeDtypeStruct((TOK, COLS), F32),
            jax.ShapeDtypeStruct((D, HID), F32),
            jax.ShapeDtypeStruct((D, HID), F32),
        ),
        in_specs=[
            pl.BlockSpec((D // steps, WIDE), lambda i: (i, 0)),
            pl.BlockSpec((TOK // steps, COLS), lambda i: (i, 0)),
            pl.BlockSpec((TOK // steps, COLS), lambda i: (i, 0)),
        ],
        out_specs=(
            pl.BlockSpec((TOK // steps, COLS), lambda i: (i, 0)),
            pl.BlockSpec((D // steps, HID), lambda i: (i, 0)),
            pl.BlockSpec((D // steps, HID), lambda i: (i, 0)),
        ),
        cost_estimate=pl.CostEstimate(flops=10**7, bytes_accessed=10**7, transcendentals=0),
    )(w, own, last)


def body(*args):
    return finish(*exchange(*args))


def solution(mesh):
    spread = ("row", "col")
    in_specs = (P("dp", spread),) * 4 + (P(None, spread),) * 2
    out_specs = (P("dp", spread), P(None, spread), P(None, spread))
    return jax.shard_map(body, mesh=mesh, in_specs=in_specs, out_specs=out_specs, check_vma=False)
```

```python
import functools

import jax
import jax.numpy as jnp
from jax import lax
from jax.experimental import pallas as pl
from jax.experimental.pallas import tpu as pltpu
from jax.sharding import PartitionSpec as P

ROOT_TWO_PI = 0.7978845608028654
CUBIC = 0.044715
MESH = pl.DeviceIdType.MESH
F32, BF16 = jnp.float32, jnp.bfloat16

TOK = 1024
HID = 320
WIDE = 2 * HID
COLS = 128
D = 2048
CHUNKS = 8
XR = WIDE // 4
ZR = XR // 2


def geglu_grads(gate_input, up_input, hidden_grad):
    gate_pre = gate_input.astype(F32)
    up_pre = up_input.astype(F32)
    grad_hidden = hidden_grad.astype(F32)
    tanh_part = jnp.tanh(ROOT_TWO_PI * (gate_pre + CUBIC * gate_pre * gate_pre * gate_pre))
    gelu_value = 0.5 * gate_pre * (1.0 + tanh_part)
    gelu_slope = 0.5 * (1.0 + tanh_part) + 0.5 * gate_pre * (
        1.0 - tanh_part * tanh_part
    ) * ROOT_TWO_PI * (1.0 + 3.0 * CUBIC * gate_pre * gate_pre)
    return (grad_hidden * up_pre * gelu_slope).astype(BF16), (grad_hidden * gelu_value).astype(BF16)


def kernel(
    act_h, gate_h, up_h, hid_h, wg_h, wu_h,
    w_out, own_out, last_out,
    gate_v, up_v, hid_v, wp, gp_t, gp, ag,
    part, xs, xr, x3, qs, q1, zr, z3, z3r,
    pkeep, bs, br, ykeep, ys, yr, y3, tz,
    in_sem, ag_recv, ag_send, c_recv, c_send, b_recv, b_send, y_recv, y_send, t_recv, t_send,
):
    dp, row, col = lax.axis_index("dp"), lax.axis_index("row"), lax.axis_index("col")
    zh, x = dp // 4, lax.rem(dp, 4)
    y, core = col // 2, lax.rem(col, 2)
    s = 2 * core - 1

    def at(base, step):
        return lax.rem(base + step + 4, 4)

    def dev(dx=0, dzh=0, dy=0, flip_row=False, flip_core=False):
        return (
            at(zh, dzh) * 4 + at(x, dx),
            1 - row if flip_row else row,
            at(y, dy) * 2 + (1 - core if flip_core else core),
        )

    x_up, x_down = dev(dx=s), dev(dx=-s)
    z_up, z_down = dev(dzh=s), dev(dzh=-s)
    y_up, y_down = dev(dy=s), dev(dy=-s)
    pair, mate = dev(flip_row=True), dev(flip_core=True)

    def place(other_row, dy, other_core=False):
        return (1 - row if other_row else row) * 8 + at(y, dy) * 2 + (1 - core if other_core else core)

    own = place(False, 0)
    loads = []
    for n, (src, dst) in enumerate(
        (
            (act_h, ag.at[own]), (gate_h, gate_v), (up_h, up_v), (hid_h, hid_v),
            (wg_h, wp.at[0:HID]), (wu_h, wp.at[HID:WIDE]),
        )
    ):
        loads.append(pltpu.make_async_copy(src, dst, in_sem.at[n]))
        loads[-1].start()

    barrier = pltpu.get_barrier_semaphore()
    for other in (x_up, x_down, z_up, z_down, y_up, y_down, pair, mate):
        pl.semaphore_signal(barrier, inc=1, device_id=other, device_id_type=MESH)

    sent = []

    def send(src, dst, send_sem, recv_sem, to):
        copy = pltpu.make_async_remote_copy(
            src_ref=src, dst_ref=dst, send_sem=send_sem, recv_sem=recv_sem,
            device_id=to, device_id_type=MESH,
        )
        copy.start()
        sent.append(copy)

    def arrived(dst, recv_sem, send_sem):
        pltpu.make_async_remote_copy(
            src_ref=dst, dst_ref=dst, send_sem=send_sem, recv_sem=recv_sem,
            device_id=mate, device_id_type=MESH,
        ).wait_recv()

    n_ag = [0]

    def ag_give(slot, to):
        send(ag.at[slot], ag.at[slot], ag_send.at[n_ag[0]], ag_recv.at[slot], to)
        n_ag[0] += 1

    def ag_take(slot):
        arrived(ag.at[slot], ag_recv.at[slot], ag_send.at[0])

    loads[0].wait()
    pl.semaphore_wait(barrier, 8)
    for to in (pair, y_up, y_down, mate):
        ag_give(own, to)

    for load in loads[1:4]:
        load.wait()

    def gate_rows(i, carry):
        rows = pl.ds(pl.multiple_of(i * 16, 16), 16)
        gate_grad, up_grad = geglu_grads(gate_v[rows, :], up_v[rows, :], hid_v[rows, :])
        gp_t[rows, :] = gate_grad
        gp_t[pl.ds(pl.multiple_of(HID + i * 16, 16), 16), :] = up_grad
        return carry

    lax.fori_loop(0, HID // 16, gate_rows, 0)

    order = ((False, 0), (True, 0), (False, -s), (False, s), (True, -s), (True, s), (False, 2), (True, 2))

    def first_block(k):
        other_row, dy = order[k]
        return (1 - row if other_row else row) * 8 + at(y, dy) * 2

    def c_give(k, n, src, dst, to):
        send(src, dst, c_send.at[k, n], c_recv.at[k, n], to)

    def c_take(k, n, dst):
        arrived(dst, c_recv.at[k, n], c_send.at[k, n])

    def x_rows(place_x):
        return pl.ds(pl.multiple_of(place_x * XR, XR), XR)

    def c0(k):
        other_row, dy = order[k]
        ag_take(place(other_row, dy, True))
        first = first_block(k)
        both = jnp.concatenate([ag[first], ag[first + 1]], axis=1)
        sums = jnp.dot(gp_t[...], both, preferred_element_type=F32)
        part[k, 0] = sums[:, 0:COLS]
        part[k, 1] = sums[:, COLS : 2 * COLS]
        xs[k, 0] = part[k, :, x_rows(at(x, 2)), :].astype(BF16)
        c_give(k, 0, xs.at[k, 0], xr.at[k, 0], x_up)
        xs[k, 1] = part[k, :, x_rows(at(x, -s)), :].astype(BF16)
        c_give(k, 1, xs.at[k, 1], xr.at[k, 1], x_down)

    def c1(k):
        c_take(k, 0, xr.at[k, 0])
        x3[k] = (part[k, :, x_rows(at(x, s)), :] + xr[k, 0].astype(F32)).astype(BF16)
        c_give(k, 2, x3.at[k], xr.at[k, 2], x_up)

    def c2(k):
        c_take(k, 1, xr.at[k, 1])
        c_take(k, 2, xr.at[k, 2])
        q1[k] = part[k, :, x_rows(x), :] + xr[k, 1].astype(F32) + xr[k, 2].astype(F32)
        qs[k, 0] = z_part(k, at(zh, 2)).astype(BF16)
        c_give(k, 3, qs.at[k, 0], zr.at[k, 0], z_up)
        qs[k, 1] = z_part(k, at(zh, -s)).astype(BF16)
        c_give(k, 4, qs.at[k, 1], zr.at[k, 1], z_down)

    def z_part(k, place_z):
        return q1[k, place_z // 2, pl.ds(pl.multiple_of(lax.rem(place_z, 2) * ZR, ZR), ZR), :]

    def c3(k):
        c_take(k, 3, zr.at[k, 0])
        z3[k] = z_part(k, at(zh, s)) + zr[k, 0].astype(F32)
        c_give(k, 5, z3.at[k], z3r.at[k], z_up)

    def out_x(k, place_x):
        return w_out.at[pl.ds(first_block(k), 2), x_rows(place_x), :]

    def out_z(k, place_z):
        rows = pl.ds(pl.multiple_of(x * XR + lax.rem(place_z, 2) * ZR, ZR), ZR)
        return w_out.at[first_block(k) + place_z // 2, rows, :]

    def c4(k):
        c_take(k, 4, zr.at[k, 1])
        c_take(k, 5, z3r.at[k])
        total = z_part(k, zh) + zr[k, 1].astype(F32) + z3r[k]
        mine = out_z(k, zh)
        mine[...] = total.astype(BF16)
        c_give(k, 6, mine, mine, z_up)
        c_give(k, 7, mine, mine, z_down)

    def c5(k):
        got = out_z(k, at(zh, -s))
        c_take(k, 6, got)
        c_give(k, 8, got, got, z_up)

    def c6(k):
        c_take(k, 7, out_z(k, at(zh, s)))
        c_take(k, 8, out_z(k, at(zh, 2)))
        mine = out_x(k, x)
        c_give(k, 9, mine, mine, x_up)
        c_give(k, 10, mine, mine, x_down)

    def c7(k):
        got = out_x(k, at(x, -s))
        c_take(k, 9, got)
        c_give(k, 11, got, got, x_up)

    def c8(k):
        c_take(k, 10, out_x(k, at(x, s)))
        c_take(k, 11, out_x(k, at(x, 2)))

    def ag_pair():
        slot = place(True, 0)
        ag_take(slot)
        for to in (y_up, y_down, mate):
            ag_give(slot, to)

    def ag_near(other_row):
        slot = place(other_row, -s)
        ag_take(slot)
        ag_give(slot, y_up)
        ag_give(slot, mate)
        slot = place(other_row, s)
        ag_take(slot)
        ag_give(slot, mate)

    def ag_far(other_row):
        slot = place(other_row, 2)
        ag_take(slot)
        ag_give(slot, mate)

    def flip():
        loads[4].wait()
        loads[5].wait()
        for i in range(TOK // 128):
            rows = slice(i * 128, i * 128 + 128)
            gp[rows, :] = gp_t[:, rows].T

    def b0(i):
        first = ((i // 4) * 8 + at(y, i % 4) * 2) * COLS
        mine = wp[:, pl.ds(pl.multiple_of(first + core * COLS, COLS), COLS)]
        others = wp[:, pl.ds(pl.multiple_of(first + (1 - core) * COLS, COLS), COLS)]
        both = jnp.concatenate([mine, others], axis=1)

        def step(r, carry):
            rows = pl.ds(pl.multiple_of(r * 256, 256), 256)
            sums = jnp.dot(gp[rows, :], both, preferred_element_type=F32)
            pkeep[i, rows, :] = sums[:, 0:COLS]
            bs[i, rows, :] = sums[:, COLS : 2 * COLS].astype(BF16)
            return carry

        lax.fori_loop(0, TOK // 256, step, 0)
        send(bs.at[i], br.at[i], b_send.at[i], b_recv.at[i], mate)

    def b1(r):
        for i in range(4 * r, 4 * r + 4):
            arrived(br.at[i], b_recv.at[i], b_send.at[i])

        def pair_sum(off):
            i = 4 * r + at(0, off)
            return pkeep[i] + br[i].astype(F32)

        ys[r, 0] = pair_sum(2).astype(BF16)
        send(ys.at[r, 0], yr.at[r, 0], y_send.at[r, 0], y_recv.at[r, 0], y_up)
        ys[r, 1] = pair_sum(-s).astype(BF16)
        send(ys.at[r, 1], yr.at[r, 1], y_send.at[r, 1], y_recv.at[r, 1], y_down)
        ykeep[r, 0] = pair_sum(s)
        ykeep[r, 1] = pair_sum(0)

    def b2(r):
        arrived(yr.at[r, 0], y_recv.at[r, 0], y_send.at[r, 0])
        y3[r] = (ykeep[r, 0] + yr[r, 0].astype(F32)).astype(BF16)
        send(y3.at[r], yr.at[r, 2], y_send.at[r, 2], y_recv.at[r, 2], y_up)

    def b3():
        for r in range(2):
            for n in (1, 2):
                arrived(yr.at[r, n], y_recv.at[r, n], y_send.at[r, n])

        def total(r):
            return ykeep[r, 1] + yr[r, 1].astype(F32) + yr[r, 2].astype(F32)

        tz[...] = total(1 - row).astype(BF16)
        send(tz, last_out, t_send, t_recv, pair)
        own_out[...] = total(row)

    def b4():
        arrived(last_out, t_recv, t_send)

    extra = {
        0: (flip, lambda: b0(0), lambda: b0(1), lambda: b0(2), lambda: b0(3), ag_pair),
        1: (lambda: ag_near(False), lambda: b0(4), lambda: b0(5)),
        2: (lambda: b0(6), lambda: b0(7)),
        3: (),
        4: (lambda: ag_near(True),),
        5: (lambda: b1(0), lambda: b1(1)),
        6: (lambda: ag_far(False),),
        7: (lambda: ag_far(True),),
        8: (lambda: b2(0), lambda: b2(1)),
        12: (b3,),
    }
    stages = (c0, c1, c2, c3, c4, c5, c6, c7, c8)
    before = {2, 4, 6, 7}
    for t in range(CHUNKS + len(stages) - 1):
        if t in before:
            for f in extra.get(t, ()):
                f()
        for n in range(len(stages) - 1, -1, -1):
            if 0 <= t - n < CHUNKS:
                stages[n](t - n)
        if t not in before:
            for f in extra.get(t, ()):
                f()
    b4()
    for copy in sent:
        copy.wait_send()


def exchange(*args):
    vmem = pltpu.VMEM
    dma = pltpu.SemaphoreType.DMA
    return pl.pallas_call(
        kernel,
        name="exchange",
        out_shape=(
            jax.ShapeDtypeStruct((16, WIDE, COLS), BF16),
            jax.ShapeDtypeStruct((TOK, COLS), F32),
            jax.ShapeDtypeStruct((TOK, COLS), BF16),
        ),
        in_specs=[pl.BlockSpec(memory_space=pl.ANY)] * 6,
        out_specs=[pl.BlockSpec(memory_space=pltpu.VMEM)] * 3,
        scratch_shapes=[
            vmem((HID, TOK), BF16), vmem((HID, TOK), BF16), vmem((HID, TOK), BF16),
            vmem((WIDE, D), BF16), vmem((WIDE, TOK), BF16), vmem((TOK, WIDE), BF16), vmem((16, TOK, COLS), BF16),
            vmem((CHUNKS, 2, WIDE, COLS), F32), vmem((CHUNKS, 2, 2, XR, COLS), BF16),
            vmem((CHUNKS, 3, 2, XR, COLS), BF16), vmem((CHUNKS, 2, XR, COLS), BF16),
            vmem((CHUNKS, 2, ZR, COLS), BF16), vmem((CHUNKS, 2, XR, COLS), F32),
            vmem((CHUNKS, 2, ZR, COLS), BF16), vmem((CHUNKS, ZR, COLS), F32), vmem((CHUNKS, ZR, COLS), F32),
            vmem((8, TOK, COLS), F32), vmem((8, TOK, COLS), BF16), vmem((8, TOK, COLS), BF16),
            vmem((2, 2, TOK, COLS), F32), vmem((2, 2, TOK, COLS), BF16), vmem((2, 3, TOK, COLS), BF16),
            vmem((2, TOK, COLS), BF16), vmem((TOK, COLS), BF16),
            dma((6,)), dma((16,)), dma((16,)), dma((CHUNKS, 12)), dma((CHUNKS, 12)), dma((8,)), dma((8,)),
            dma((2, 3)), dma((2, 3)), dma, dma,
        ],
        compiler_params=pltpu.CompilerParams(
            collective_id=0, has_side_effects=True, vmem_limit_bytes=63 * 1024 * 1024
        ),
        cost_estimate=pl.CostEstimate(flops=5 * 10**9, bytes_accessed=10**7, transcendentals=0),
    )(*args)


def finish_kernel(w_ref, own_ref, last_ref, x_ref, gate_ref, up_ref):
    for n in range(2):
        cols = slice(n * COLS, (n + 1) * COLS)
        gate_ref[:, cols] = w_ref[n, 0:HID, :].astype(F32)
        up_ref[:, cols] = w_ref[n, HID:WIDE, :].astype(F32)
    x_ref[...] = own_ref[...] + last_ref[...].astype(F32)


def finish(w, own, last):
    steps = 8
    return pl.pallas_call(
        finish_kernel,
        name="finish",
        grid=(steps,),
        out_shape=(
            jax.ShapeDtypeStruct((TOK, COLS), F32),
            jax.ShapeDtypeStruct((HID, D), F32),
            jax.ShapeDtypeStruct((HID, D), F32),
        ),
        in_specs=[
            pl.BlockSpec((2, WIDE, COLS), lambda i: (i, 0, 0)),
            pl.BlockSpec((TOK // steps, COLS), lambda i: (i, 0)),
            pl.BlockSpec((TOK // steps, COLS), lambda i: (i, 0)),
        ],
        out_specs=(
            pl.BlockSpec((TOK // steps, COLS), lambda i: (i, 0)),
            pl.BlockSpec((HID, 2 * COLS), lambda i: (0, i)),
            pl.BlockSpec((HID, 2 * COLS), lambda i: (0, i)),
        ),
        cost_estimate=pl.CostEstimate(flops=10**7, bytes_accessed=10**7, transcendentals=0),
    )(w, own, last)


def body(activations, *others):
    input_grad, gate_t, up_t = finish(*exchange(activations, *(a.T for a in others)))
    return input_grad, gate_t.T, up_t.T


def solution(mesh):
    spread = ("row", "col")
    in_specs = (P("dp", spread),) * 4 + (P(None, spread),) * 2
    out_specs = (P("dp", spread), P(None, spread), P(None, spread))
    return jax.shard_map(body, mesh=mesh, in_specs=in_specs, out_specs=out_specs, check_vma=False)
```

```python
import functools

import jax
import jax.numpy as jnp
from jax import lax
from jax.experimental import pallas as pl
from jax.experimental.pallas import tpu as pltpu
from jax.sharding import PartitionSpec as P

ROOT_TWO_PI = 0.7978845608028654
CUBIC = 0.044715
MESH = pl.DeviceIdType.MESH
F32, BF16 = jnp.float32, jnp.bfloat16

TOK = 1024
HID = 320
WIDE = 2 * HID
COLS = 128
D = 2048
STEPS = 2
CHUNKS = 8
XR = WIDE // 4
ZR = XR // 2


ORDER = (
    ("c0", 0), ("flip",), ("ag_pair",), ("b0", 7), ("b0", 3), ("c1", 0), ("ag_nearm", 0), ("ag_nearp", 0), ("c0", 1),
    ("b0", 4), ("c0", 3), ("c2", 0), ("b0", 6), ("c0", 2), ("b0", 1), ("c1", 3), ("c1", 1), ("ag_nearp", 1),
    ("c3", 0), ("b0", 2), ("ag_nearm", 1), ("c1", 2), ("c0", 4), ("ag_far", 0), ("c2", 3), ("b0", 5), ("c4", 0),
    ("c2", 1), ("c0", 6), ("c0", 5), ("ag_far", 1), ("c2", 2), ("c3", 3), ("b1", 1), ("c1", 4), ("c5", 0), ("c1", 6),
    ("c3", 1), ("b0", 0), ("c3", 2), ("c0", 7), ("c4", 3), ("c1", 5), ("c2", 4), ("c2", 6), ("c4", 2), ("c1", 7),
    ("c5", 3), ("c4", 1), ("b1", 0), ("c2", 5), ("c6", 0), ("c3", 6), ("b2", 1), ("c5", 2), ("c2", 7), ("c6", 3),
    ("c5", 1), ("c3", 5), ("c3", 4), ("c7", 0), ("c6", 2), ("c4", 6), ("c6", 1), ("c3", 7), ("c4", 5), ("c4", 4),
    ("c5", 6), ("c7", 3), ("c8", 0), ("c7", 2), ("c4", 7), ("c5", 5), ("b2", 0), ("c7", 1), ("c5", 4), ("c6", 6),
    ("c5", 7), ("c6", 5), ("c6", 4), ("c8", 2), ("c6", 7), ("c7", 6), ("c8", 3), ("b3",), ("c7", 4), ("c7", 5),
    ("c7", 7), ("c8", 1), ("c8", 4), ("b4",), ("c8", 6), ("c8", 5), ("c8", 7),
)


def geglu_grads(gate_input, up_input, hidden_grad):
    gate_pre = gate_input.astype(F32)
    up_pre = up_input.astype(F32)
    grad_hidden = hidden_grad.astype(F32)
    tanh_part = jnp.tanh(ROOT_TWO_PI * (gate_pre + CUBIC * gate_pre * gate_pre * gate_pre))
    gelu_value = 0.5 * gate_pre * (1.0 + tanh_part)
    gelu_slope = 0.5 * (1.0 + tanh_part) + 0.5 * gate_pre * (
        1.0 - tanh_part * tanh_part
    ) * ROOT_TWO_PI * (1.0 + 3.0 * CUBIC * gate_pre * gate_pre)
    return (grad_hidden * up_pre * gelu_slope).astype(BF16), (grad_hidden * gelu_value).astype(BF16)


def kernel(
    act_h, gate_h, up_h, hid_h, wg_h, wu_h,
    w_out, own_out, last_out,
    gate_v, up_v, hid_v, wp, gp_t, gp, ag,
    part, xs, xr, x3, qs, q1, zr, z3, z3r,
    pkeep, bs, br, ykeep, ys, yr, y3, tz,
    in_sem, ag_recv, ag_send, c_recv, c_send, b_recv, b_send, y_recv, y_send, t_recv, t_send,
):
    dp, row, col = lax.axis_index("dp"), lax.axis_index("row"), lax.axis_index("col")
    zh, x = dp // 4, lax.rem(dp, 4)
    y, core = col // 2, lax.rem(col, 2)
    s = 2 * core - 1

    def at(base, step):
        return lax.rem(base + step + 4, 4)

    def dev(dx=0, dzh=0, dy=0, flip_row=False, flip_core=False):
        return (
            at(zh, dzh) * 4 + at(x, dx),
            1 - row if flip_row else row,
            at(y, dy) * 2 + (1 - core if flip_core else core),
        )

    x_up, x_down = dev(dx=s), dev(dx=-s)
    z_up, z_down = dev(dzh=s), dev(dzh=-s)
    y_up, y_down = dev(dy=s), dev(dy=-s)
    pair, mate = dev(flip_row=True), dev(flip_core=True)

    def place(other_row, dy, other_core=False):
        return (1 - row if other_row else row) * 8 + at(y, dy) * 2 + (1 - core if other_core else core)

    own = place(False, 0)
    loads = []
    for n, (src, dst) in enumerate(
        (
            (act_h, ag.at[own]), (gate_h, gate_v), (up_h, up_v), (hid_h, hid_v),
            (wg_h, wp.at[0:HID]), (wu_h, wp.at[HID:WIDE]),
        )
    ):
        loads.append(pltpu.make_async_copy(src, dst, in_sem.at[n]))
        loads[-1].start()

    barrier = pltpu.get_barrier_semaphore()
    for other in (x_up, x_down, z_up, z_down, y_up, y_down, pair, mate):
        pl.semaphore_signal(barrier, inc=1, device_id=other, device_id_type=MESH)

    sent = []

    def send(src, dst, send_sem, recv_sem, to):
        copy = pltpu.make_async_remote_copy(
            src_ref=src, dst_ref=dst, send_sem=send_sem, recv_sem=recv_sem,
            device_id=to, device_id_type=MESH,
        )
        copy.start()
        sent.append(copy)

    def arrived(dst, recv_sem, send_sem):
        pltpu.make_async_remote_copy(
            src_ref=dst, dst_ref=dst, send_sem=send_sem, recv_sem=recv_sem,
            device_id=mate, device_id_type=MESH,
        ).wait_recv()

    n_ag = [0]

    def ag_give(slot, to):
        send(ag.at[slot], ag.at[slot], ag_send.at[n_ag[0]], ag_recv.at[slot], to)
        n_ag[0] += 1

    def ag_take(slot):
        arrived(ag.at[slot], ag_recv.at[slot], ag_send.at[0])

    loads[0].wait()
    pl.semaphore_wait(barrier, 8)
    for to in (pair, y_up, y_down, mate):
        ag_give(own, to)

    for load in loads[1:4]:
        load.wait()

    def gate_rows(i, carry):
        rows = pl.ds(pl.multiple_of(i * 16, 16), 16)
        gate_grad, up_grad = geglu_grads(gate_v[rows, :], up_v[rows, :], hid_v[rows, :])
        gp_t[rows, :] = gate_grad
        gp_t[pl.ds(pl.multiple_of(HID + i * 16, 16), 16), :] = up_grad
        return carry

    lax.fori_loop(0, HID // 16, gate_rows, 0)

    order = ((False, 0), (True, 0), (False, -s), (False, s), (True, -s), (True, s), (False, 2), (True, 2))

    def first_block(k):
        other_row, dy = order[k]
        return (1 - row if other_row else row) * 8 + at(y, dy) * 2

    def c_give(k, n, src, dst, to):
        send(src, dst, c_send.at[k, n], c_recv.at[k, n], to)

    def c_take(k, n, dst):
        arrived(dst, c_recv.at[k, n], c_send.at[k, n])

    def x_rows(place_x):
        return pl.ds(pl.multiple_of(place_x * XR, XR), XR)

    def c0(k):
        other_row, dy = order[k]
        ag_take(place(other_row, dy, True))
        first = first_block(k)
        both = jnp.concatenate([ag[first], ag[first + 1]], axis=1)
        sums = jnp.dot(gp_t[...], both, preferred_element_type=F32)
        part[k, 0] = sums[:, 0:COLS]
        part[k, 1] = sums[:, COLS : 2 * COLS]
        xs[k, 0] = part[k, :, x_rows(at(x, 2)), :].astype(BF16)
        c_give(k, 0, xs.at[k, 0], xr.at[k, 0], x_up)
        xs[k, 1] = part[k, :, x_rows(at(x, -s)), :].astype(BF16)
        c_give(k, 1, xs.at[k, 1], xr.at[k, 1], x_down)

    def c1(k):
        c_take(k, 0, xr.at[k, 0])
        x3[k] = (part[k, :, x_rows(at(x, s)), :] + xr[k, 0].astype(F32)).astype(BF16)
        c_give(k, 2, x3.at[k], xr.at[k, 2], x_up)

    def c2(k):
        c_take(k, 1, xr.at[k, 1])
        c_take(k, 2, xr.at[k, 2])
        q1[k] = part[k, :, x_rows(x), :] + xr[k, 1].astype(F32) + xr[k, 2].astype(F32)
        qs[k, 0] = z_part(k, at(zh, 2)).astype(BF16)
        c_give(k, 3, qs.at[k, 0], zr.at[k, 0], z_up)
        qs[k, 1] = z_part(k, at(zh, -s)).astype(BF16)
        c_give(k, 4, qs.at[k, 1], zr.at[k, 1], z_down)

    def z_part(k, place_z):
        return q1[k, place_z // 2, pl.ds(pl.multiple_of(lax.rem(place_z, 2) * ZR, ZR), ZR), :]

    def c3(k):
        c_take(k, 3, zr.at[k, 0])
        z3[k] = z_part(k, at(zh, s)) + zr[k, 0].astype(F32)
        c_give(k, 5, z3.at[k], z3r.at[k], z_up)

    def out_x(k, place_x):
        return w_out.at[pl.ds(first_block(k), 2), x_rows(place_x), :]

    def out_z(k, place_z):
        rows = pl.ds(pl.multiple_of(x * XR + lax.rem(place_z, 2) * ZR, ZR), ZR)
        return w_out.at[first_block(k) + place_z // 2, rows, :]

    def c4(k):
        c_take(k, 4, zr.at[k, 1])
        c_take(k, 5, z3r.at[k])
        total = z_part(k, zh) + zr[k, 1].astype(F32) + z3r[k]
        mine = out_z(k, zh)
        mine[...] = total.astype(BF16)
        c_give(k, 6, mine, mine, z_up)
        c_give(k, 7, mine, mine, z_down)

    def c5(k):
        got = out_z(k, at(zh, -s))
        c_take(k, 6, got)
        c_give(k, 8, got, got, z_up)

    def c6(k):
        c_take(k, 7, out_z(k, at(zh, s)))
        c_take(k, 8, out_z(k, at(zh, 2)))
        mine = out_x(k, x)
        c_give(k, 9, mine, mine, x_up)
        c_give(k, 10, mine, mine, x_down)

    def c7(k):
        got = out_x(k, at(x, -s))
        c_take(k, 9, got)
        c_give(k, 11, got, got, x_up)

    def c8(k):
        c_take(k, 10, out_x(k, at(x, s)))
        c_take(k, 11, out_x(k, at(x, 2)))

    def ag_pair():
        slot = place(True, 0)
        ag_take(slot)
        for to in (y_up, y_down, mate):
            ag_give(slot, to)

    def ag_nearm(other_row):
        slot = place(other_row, -s)
        ag_take(slot)
        ag_give(slot, y_up)
        ag_give(slot, mate)

    def ag_nearp(other_row):
        slot = place(other_row, s)
        ag_take(slot)
        ag_give(slot, mate)

    def ag_far(other_row):
        slot = place(other_row, 2)
        ag_take(slot)
        ag_give(slot, mate)

    def flip():
        loads[4].wait()
        loads[5].wait()
        for i in range(TOK // 128):
            rows = slice(i * 128, i * 128 + 128)
            gp[rows, :] = gp_t[:, rows].T

    def b0(i):
        first = ((i // 4) * 8 + at(y, i % 4) * 2) * COLS
        mine = wp[:, pl.ds(pl.multiple_of(first + core * COLS, COLS), COLS)]
        others = wp[:, pl.ds(pl.multiple_of(first + (1 - core) * COLS, COLS), COLS)]
        both = jnp.concatenate([mine, others], axis=1)

        def step(r, carry):
            rows = pl.ds(pl.multiple_of(r * 256, 256), 256)
            sums = jnp.dot(gp[rows, :], both, preferred_element_type=F32)
            pkeep[i, rows, :] = sums[:, 0:COLS]
            bs[i, rows, :] = sums[:, COLS : 2 * COLS].astype(BF16)
            return carry

        lax.fori_loop(0, TOK // 256, step, 0)
        send(bs.at[i], br.at[i], b_send.at[i], b_recv.at[i], mate)

    def b1(r):
        for i in range(4 * r, 4 * r + 4):
            arrived(br.at[i], b_recv.at[i], b_send.at[i])

        def pair_sum(off):
            i = 4 * r + at(0, off)
            return pkeep[i] + br[i].astype(F32)

        ys[r, 0] = pair_sum(2).astype(BF16)
        send(ys.at[r, 0], yr.at[r, 0], y_send.at[r, 0], y_recv.at[r, 0], y_up)
        ys[r, 1] = pair_sum(-s).astype(BF16)
        send(ys.at[r, 1], yr.at[r, 1], y_send.at[r, 1], y_recv.at[r, 1], y_down)
        ykeep[r, 0] = pair_sum(s)
        ykeep[r, 1] = pair_sum(0)

    def b2(r):
        arrived(yr.at[r, 0], y_recv.at[r, 0], y_send.at[r, 0])
        y3[r] = (ykeep[r, 0] + yr[r, 0].astype(F32)).astype(BF16)
        send(y3.at[r], yr.at[r, 2], y_send.at[r, 2], y_recv.at[r, 2], y_up)

    def b3():
        for r in range(2):
            for n in (1, 2):
                arrived(yr.at[r, n], y_recv.at[r, n], y_send.at[r, n])

        def total(r):
            return ykeep[r, 1] + yr[r, 1].astype(F32) + yr[r, 2].astype(F32)

        tz[...] = total(1 - row).astype(BF16)
        send(tz, last_out, t_send, t_recv, pair)
        own_out[...] = total(row)

    def b4():
        arrived(last_out, t_recv, t_send)

    steps = dict(
        c0=c0, c1=c1, c2=c2, c3=c3, c4=c4, c5=c5, c6=c6, c7=c7, c8=c8, flip=flip, b0=b0, b1=b1, b2=b2, b3=b3, b4=b4,
        ag_pair=ag_pair, ag_nearm=ag_nearm, ag_nearp=ag_nearp, ag_far=ag_far,
    )
    for name, *n in ORDER:
        steps[name](*n)
    for copy in sent:
        copy.wait_send()


def exchange(*args):
    vmem = pltpu.VMEM
    dma = pltpu.SemaphoreType.DMA
    return pl.pallas_call(
        kernel,
        name="exchange",
        out_shape=(
            jax.ShapeDtypeStruct((16, WIDE, COLS), BF16),
            jax.ShapeDtypeStruct((TOK, COLS), F32),
            jax.ShapeDtypeStruct((TOK, COLS), BF16),
        ),
        in_specs=[pl.BlockSpec(memory_space=pl.ANY)] * 6,
        out_specs=[pl.BlockSpec(memory_space=pltpu.VMEM)] * 3,
        scratch_shapes=[
            vmem((HID, TOK), BF16), vmem((HID, TOK), BF16), vmem((HID, TOK), BF16),
            vmem((WIDE, D), BF16), vmem((WIDE, TOK), BF16), vmem((TOK, WIDE), BF16), vmem((16, TOK, COLS), BF16),
            vmem((CHUNKS, 2, WIDE, COLS), F32), vmem((CHUNKS, 2, 2, XR, COLS), BF16),
            vmem((CHUNKS, 3, 2, XR, COLS), BF16), vmem((CHUNKS, 2, XR, COLS), BF16),
            vmem((CHUNKS, 2, ZR, COLS), BF16), vmem((CHUNKS, 2, XR, COLS), F32),
            vmem((CHUNKS, 2, ZR, COLS), BF16), vmem((CHUNKS, ZR, COLS), F32), vmem((CHUNKS, ZR, COLS), F32),
            vmem((8, TOK, COLS), F32), vmem((8, TOK, COLS), BF16), vmem((8, TOK, COLS), BF16),
            vmem((2, 2, TOK, COLS), F32), vmem((2, 2, TOK, COLS), BF16), vmem((2, 3, TOK, COLS), BF16),
            vmem((2, TOK, COLS), BF16), vmem((TOK, COLS), BF16),
            dma((6,)), dma((16,)), dma((16,)), dma((CHUNKS, 12)), dma((CHUNKS, 12)), dma((8,)), dma((8,)),
            dma((2, 3)), dma((2, 3)), dma, dma,
        ],
        compiler_params=pltpu.CompilerParams(
            collective_id=0, has_side_effects=True, vmem_limit_bytes=63 * 1024 * 1024
        ),
        cost_estimate=pl.CostEstimate(flops=5 * 10**9, bytes_accessed=10**7, transcendentals=0),
    )(*args)


def finish_kernel(w_ref, own_ref, last_ref, x_ref, gate_ref, up_ref):
    for n in range(16 // STEPS):
        cols = slice(n * COLS, (n + 1) * COLS)
        gate_ref[:, cols] = w_ref[n, 0:HID, :].astype(F32)
        up_ref[:, cols] = w_ref[n, HID:WIDE, :].astype(F32)
    x_ref[...] = own_ref[...] + last_ref[...].astype(F32)


def finish(w, own, last):
    return pl.pallas_call(
        finish_kernel,
        name="finish",
        grid=(STEPS,),
        out_shape=(
            jax.ShapeDtypeStruct((TOK, COLS), F32),
            jax.ShapeDtypeStruct((HID, D), F32),
            jax.ShapeDtypeStruct((HID, D), F32),
        ),
        in_specs=[
            pl.BlockSpec((16 // STEPS, WIDE, COLS), lambda i: (i, 0, 0)),
            pl.BlockSpec((TOK // STEPS, COLS), lambda i: (i, 0)),
            pl.BlockSpec((TOK // STEPS, COLS), lambda i: (i, 0)),
        ],
        out_specs=(
            pl.BlockSpec((TOK // STEPS, COLS), lambda i: (i, 0)),
            pl.BlockSpec((HID, D // STEPS), lambda i: (0, i)),
            pl.BlockSpec((HID, D // STEPS), lambda i: (0, i)),
        ),
        cost_estimate=pl.CostEstimate(flops=10**7, bytes_accessed=10**7, transcendentals=0),
    )(w, own, last)


def body(activations, *others):
    input_grad, gate_t, up_t = finish(*exchange(activations, *(a.T for a in others)))
    return input_grad, gate_t.T, up_t.T


def solution(mesh):
    spread = ("row", "col")
    in_specs = (P("dp", spread),) * 4 + (P(None, spread),) * 2
    out_specs = (P("dp", spread), P(None, spread), P(None, spread))
    return jax.shard_map(body, mesh=mesh, in_specs=in_specs, out_specs=out_specs, check_vma=False)
```

```python
import functools

import jax
import jax.numpy as jnp
from jax import lax
from jax.experimental import pallas as pl
from jax.experimental.pallas import tpu as pltpu
from jax.sharding import PartitionSpec as P

ROOT_TWO_PI = 0.7978845608028654
CUBIC = 0.044715
MESH = pl.DeviceIdType.MESH
F32, BF16 = jnp.float32, jnp.bfloat16

TOK = 1024
HID = 320
WIDE = 2 * HID
COLS = 128
D = 2048
STEPS = 4
CHUNKS = 8
XR = WIDE // 4
ZR = XR // 2


ORDER = (
    ("c0", 0), ("flip",), ("b0", 5), ("ag_pair",), ("c1", 0), ("ag_nearp", 0), ("ag_nearm", 0), ("b0", 3), ("c0", 1),
    ("c0", 2), ("b0", 0), ("c2", 0), ("c0", 3), ("c1", 1), ("b0", 4), ("b0", 6), ("b0", 1), ("ag_nearm", 1),
    ("ag_nearp", 1), ("c4", 0), ("c1", 3), ("c1", 2), ("b0", 2), ("c2", 1), ("c0", 5), ("ag_far", 0), ("c0", 4),
    ("zin", 0, 1), ("c2", 3), ("c8", 0, 0), ("b1", 0), ("c2", 2), ("ag_far", 1), ("c1", 5), ("c4", 1), ("b0", 7),
    ("c0", 7), ("c4", 3), ("c1", 4), ("b1", 1), ("c2", 5), ("c4", 2), ("c0", 6), ("c1", 7), ("c8", 3, 0),
    ("zin", 1, 1), ("b2", 0), ("c2", 4), ("c8", 2, 0), ("zin", 0, 3), ("c4", 5), ("c1", 6), ("c2", 7), ("zin", 3, 1),
    ("c8", 0, 1), ("zin", 2, 3), ("zin", 1, 2), ("zin", 3, 2), ("zin", 0, 2), ("zin", 3, 3), ("zin", 2, 2), ("c2", 6),
    ("zin", 1, 3), ("b2", 1), ("c8", 1, 1), ("c4", 4), ("c8", 2, 3), ("c8", 5, 0), ("c8", 3, 2), ("zin", 2, 1),
    ("c8", 0, 3), ("zin", 5, 1), ("c8", 1, 0), ("c4", 7), ("c8", 1, 2), ("zin", 5, 2), ("c8", 0, 2), ("c4", 6),
    ("c8", 1, 3), ("c8", 3, 1), ("c8", 2, 2), ("zin", 4, 2), ("c8", 5, 1), ("zin", 4, 3), ("c8", 2, 1), ("zin", 5, 3),
    ("zin", 7, 2), ("c8", 6, 0), ("zin", 4, 1), ("zin", 7, 3), ("b3",), ("zin", 6, 1), ("c8", 7, 0), ("zin", 6, 3),
    ("zin", 7, 1), ("zin", 6, 2), ("c8", 4, 0), ("c8", 4, 1), ("c8", 3, 3), ("c8", 5, 2), ("c8", 7, 3), ("c8", 4, 2),
    ("c8", 4, 3), ("c8", 5, 3), ("c8", 6, 3), ("c9", 2), ("c9", 0), ("c8", 7, 1), ("c8", 7, 2), ("c9", 1),
    ("c8", 6, 1), ("c8", 6, 2), ("c9", 4), ("c9", 5), ("c9", 3), ("c9", 7), ("c9", 6), ("b4",),
)


def geglu_grads(gate_input, up_input, hidden_grad):
    gate_pre = gate_input.astype(F32)
    up_pre = up_input.astype(F32)
    grad_hidden = hidden_grad.astype(F32)
    tanh_part = jnp.tanh(ROOT_TWO_PI * (gate_pre + CUBIC * gate_pre * gate_pre * gate_pre))
    gelu_value = 0.5 * gate_pre * (1.0 + tanh_part)
    gelu_slope = 0.5 * (1.0 + tanh_part) + 0.5 * gate_pre * (
        1.0 - tanh_part * tanh_part
    ) * ROOT_TWO_PI * (1.0 + 3.0 * CUBIC * gate_pre * gate_pre)
    return (grad_hidden * up_pre * gelu_slope).astype(BF16), (grad_hidden * gelu_value).astype(BF16)


def kernel(
    act_h, gate_h, up_h, hid_h, wg_h, wu_h,
    w_hbm, own_out, last_out,
    w_out,
    gate_v, up_v, hid_v, wp, gp_t, gp, ag,
    part, xs, xr, x3, qs, q1, zr,
    pkeep, bs, br, ykeep, ys, yr, y3, tz,
    in_sem, out_sem, ag_recv, ag_send, c_recv, c_send, b_recv, b_send, y_recv, y_send, t_recv, t_send,
):
    dp, row, col = lax.axis_index("dp"), lax.axis_index("row"), lax.axis_index("col")
    zh, x = dp // 4, lax.rem(dp, 4)
    y, core = col // 2, lax.rem(col, 2)
    s = 2 * core - 1

    def at(base, step):
        return lax.rem(base + step + 4, 4)

    def dev(dx=0, dzh=0, dy=0, flip_row=False, flip_core=False):
        return (
            at(zh, dzh) * 4 + at(x, dx),
            1 - row if flip_row else row,
            at(y, dy) * 2 + (1 - core if flip_core else core),
        )

    x_up, x_down = dev(dx=s), dev(dx=-s)
    z_up, z_down = dev(dzh=s), dev(dzh=-s)
    y_up, y_down = dev(dy=s), dev(dy=-s)
    z_far = dev(dzh=2)
    pair, mate = dev(flip_row=True), dev(flip_core=True)

    def place(other_row, dy, other_core=False):
        return (1 - row if other_row else row) * 8 + at(y, dy) * 2 + (1 - core if other_core else core)

    own = place(False, 0)
    loads = []
    for n, (src, dst) in enumerate(
        (
            (act_h, ag.at[own]), (gate_h, gate_v), (up_h, up_v), (hid_h, hid_v),
            (wg_h, wp.at[0:HID]), (wu_h, wp.at[HID:WIDE]),
        )
    ):
        loads.append(pltpu.make_async_copy(src, dst, in_sem.at[n]))
        loads[-1].start()

    barrier = pltpu.get_barrier_semaphore()
    for other in (x_up, x_down, z_up, z_down, z_far, y_up, y_down, pair, mate):
        pl.semaphore_signal(barrier, inc=1, device_id=other, device_id_type=MESH)

    sent = []

    def send(src, dst, send_sem, recv_sem, to):
        copy = pltpu.make_async_remote_copy(
            src_ref=src, dst_ref=dst, send_sem=send_sem, recv_sem=recv_sem,
            device_id=to, device_id_type=MESH,
        )
        copy.start()
        sent.append(copy)

    def arrived(dst, recv_sem, send_sem):
        pltpu.make_async_remote_copy(
            src_ref=dst, dst_ref=dst, send_sem=send_sem, recv_sem=recv_sem,
            device_id=mate, device_id_type=MESH,
        ).wait_recv()

    n_ag = [0]

    def ag_give(slot, to):
        send(ag.at[slot], ag.at[slot], ag_send.at[n_ag[0]], ag_recv.at[slot], to)
        n_ag[0] += 1

    def ag_take(slot):
        arrived(ag.at[slot], ag_recv.at[slot], ag_send.at[0])

    loads[0].wait()
    pl.semaphore_wait(barrier, 9)
    for to in (pair, y_up, y_down, mate):
        ag_give(own, to)

    for load in loads[1:4]:
        load.wait()

    def gate_rows(i, carry):
        rows = pl.ds(pl.multiple_of(i * 16, 16), 16)
        gate_grad, up_grad = geglu_grads(gate_v[rows, :], up_v[rows, :], hid_v[rows, :])
        gp_t[rows, :] = gate_grad
        gp_t[pl.ds(pl.multiple_of(HID + i * 16, 16), 16), :] = up_grad
        return carry

    lax.fori_loop(0, HID // 16, gate_rows, 0)

    order = ((False, 0), (True, 0), (False, -s), (False, s), (True, -s), (True, s), (False, 2), (True, 2))

    def first_block(k):
        other_row, dy = order[k]
        return (1 - row if other_row else row) * 8 + at(y, dy) * 2

    def c_give(k, n, src, dst, to):
        send(src, dst, c_send.at[k, n], c_recv.at[k, n], to)

    def c_take(k, n, dst):
        arrived(dst, c_recv.at[k, n], c_send.at[k, n])

    def x_rows(place_x):
        return pl.ds(pl.multiple_of(place_x * XR, XR), XR)

    def c0(k):
        other_row, dy = order[k]
        ag_take(place(other_row, dy, True))
        first = first_block(k)
        both = jnp.concatenate([ag[first], ag[first + 1]], axis=1)
        sums = jnp.dot(gp_t[...], both, preferred_element_type=F32)
        part[k, 0] = sums[:, 0:COLS]
        part[k, 1] = sums[:, COLS : 2 * COLS]
        xs[k, 0] = part[k, :, x_rows(at(x, 2)), :].astype(BF16)
        c_give(k, 0, xs.at[k, 0], xr.at[k, 0], x_up)
        xs[k, 1] = part[k, :, x_rows(at(x, -s)), :].astype(BF16)
        c_give(k, 1, xs.at[k, 1], xr.at[k, 1], x_down)

    def c1(k):
        c_take(k, 0, xr.at[k, 0])
        x3[k] = (part[k, :, x_rows(at(x, s)), :] + xr[k, 0].astype(F32)).astype(BF16)
        c_give(k, 2, x3.at[k], xr.at[k, 2], x_up)

    def c2(k):
        c_take(k, 1, xr.at[k, 1])
        c_take(k, 2, xr.at[k, 2])
        q1[k] = part[k, :, x_rows(x), :] + xr[k, 1].astype(F32) + xr[k, 2].astype(F32)
        for n, (step, to) in enumerate(((2, z_far), (-s, z_down), (s, z_up))):
            qs[k, n] = z_part(k, at(zh, step)).astype(BF16)
            c_give(k, 3 + n, qs.at[k, n], zr.at[k, n], to)

    def z_part(k, place_z):
        return q1[k, place_z // 2, pl.ds(pl.multiple_of(lax.rem(place_z, 2) * ZR, ZR), ZR), :]

    def out_part(k, place_x, place_z):
        rows = pl.ds(pl.multiple_of(place_x * XR + lax.rem(place_z, 2) * ZR, ZR), ZR)
        return w_out.at[first_block(k) + place_z // 2, rows, :]

    z_from = (0, -s, s, 2)

    def c4(k):
        for n in range(3):
            c_take(k, 3 + n, zr.at[k, n])
        total = z_part(k, zh) + zr[k, 0].astype(F32) + zr[k, 1].astype(F32) + zr[k, 2].astype(F32)
        mine = out_part(k, x, zh)
        mine[...] = total.astype(BF16)
        for n, to in enumerate((z_up, z_down, z_far)):
            c_give(k, 6 + n, mine, mine, to)
        along_x(k, 0)

    def along_x(k, j):
        held = out_part(k, x, at(zh, z_from[j]))
        c_give(k, 9 + j, held, held, x_up)
        c_give(k, 13 + j, held, held, x_down)

    def z_part_in(k, j):
        c_take(k, 5 + j, out_part(k, x, at(zh, z_from[j])))
        along_x(k, j)

    def c8(k, j):
        got = out_part(k, at(x, -s), at(zh, z_from[j]))
        c_take(k, 9 + j, got)
        c_give(k, 17 + j, got, got, x_up)

    def save(k):
        pair_of = pl.ds(first_block(k), 2)
        return pltpu.make_async_copy(w_out.at[pair_of], w_hbm.at[pair_of], out_sem.at[k])

    def c9(k):
        for j in range(4):
            c_take(k, 13 + j, out_part(k, at(x, s), at(zh, z_from[j])))
            c_take(k, 17 + j, out_part(k, at(x, 2), at(zh, z_from[j])))
        save(k).start()

    def ag_pair():
        slot = place(True, 0)
        ag_take(slot)
        for to in (y_up, y_down, mate):
            ag_give(slot, to)

    def ag_nearm(other_row):
        slot = place(other_row, -s)
        ag_take(slot)
        ag_give(slot, y_up)
        ag_give(slot, mate)

    def ag_nearp(other_row):
        slot = place(other_row, s)
        ag_take(slot)
        ag_give(slot, mate)

    def ag_far(other_row):
        slot = place(other_row, 2)
        ag_take(slot)
        ag_give(slot, mate)

    def flip():
        loads[4].wait()
        loads[5].wait()
        for i in range(TOK // 128):
            rows = slice(i * 128, i * 128 + 128)
            gp[rows, :] = gp_t[:, rows].T

    def b0(i):
        first = ((i // 4) * 8 + at(y, i % 4) * 2) * COLS
        mine = wp[:, pl.ds(pl.multiple_of(first + core * COLS, COLS), COLS)]
        others = wp[:, pl.ds(pl.multiple_of(first + (1 - core) * COLS, COLS), COLS)]
        both = jnp.concatenate([mine, others], axis=1)

        def step(r, carry):
            rows = pl.ds(pl.multiple_of(r * 256, 256), 256)
            sums = jnp.dot(gp[rows, :], both, preferred_element_type=F32)
            pkeep[i, rows, :] = sums[:, 0:COLS]
            bs[i, rows, :] = sums[:, COLS : 2 * COLS].astype(BF16)
            return carry

        lax.fori_loop(0, TOK // 256, step, 0)
        send(bs.at[i], br.at[i], b_send.at[i], b_recv.at[i], mate)

    def b1(r):
        for i in range(4 * r, 4 * r + 4):
            arrived(br.at[i], b_recv.at[i], b_send.at[i])

        def pair_sum(off):
            i = 4 * r + at(0, off)
            return pkeep[i] + br[i].astype(F32)

        ys[r, 0] = pair_sum(2).astype(BF16)
        send(ys.at[r, 0], yr.at[r, 0], y_send.at[r, 0], y_recv.at[r, 0], y_up)
        ys[r, 1] = pair_sum(-s).astype(BF16)
        send(ys.at[r, 1], yr.at[r, 1], y_send.at[r, 1], y_recv.at[r, 1], y_down)
        ykeep[r, 0] = pair_sum(s)
        ykeep[r, 1] = pair_sum(0)

    def b2(r):
        arrived(yr.at[r, 0], y_recv.at[r, 0], y_send.at[r, 0])
        y3[r] = (ykeep[r, 0] + yr[r, 0].astype(F32)).astype(BF16)
        send(y3.at[r], yr.at[r, 2], y_send.at[r, 2], y_recv.at[r, 2], y_up)

    def b3():
        for r in range(2):
            for n in (1, 2):
                arrived(yr.at[r, n], y_recv.at[r, n], y_send.at[r, n])

        def total(r):
            return ykeep[r, 1] + yr[r, 1].astype(F32) + yr[r, 2].astype(F32)

        tz[...] = total(1 - row).astype(BF16)
        send(tz, last_out, t_send, t_recv, pair)
        own_out[...] = total(row)

    def b4():
        arrived(last_out, t_recv, t_send)

    steps = dict(
        c0=c0, c1=c1, c2=c2, c4=c4, zin=z_part_in, c8=c8, c9=c9, flip=flip, b0=b0, b1=b1, b2=b2, b3=b3, b4=b4,
        ag_pair=ag_pair, ag_nearm=ag_nearm, ag_nearp=ag_nearp, ag_far=ag_far,
    )
    for name, *n in ORDER:
        steps[name](*n)
    for copy in sent:
        copy.wait_send()
    for k in range(CHUNKS):
        save(k).wait()


def exchange(*args):
    vmem = pltpu.VMEM
    dma = pltpu.SemaphoreType.DMA
    return pl.pallas_call(
        kernel,
        name="exchange",
        out_shape=(
            jax.ShapeDtypeStruct((16, WIDE, COLS), BF16),
            jax.ShapeDtypeStruct((TOK, COLS), F32),
            jax.ShapeDtypeStruct((TOK, COLS), BF16),
        ),
        in_specs=[pl.BlockSpec(memory_space=pl.ANY)] * 6,
        out_specs=[pl.BlockSpec(memory_space=pl.ANY)] + [pl.BlockSpec(memory_space=pltpu.VMEM)] * 2,
        scratch_shapes=[
            vmem((16, WIDE, COLS), BF16),
            vmem((HID, TOK), BF16), vmem((HID, TOK), BF16), vmem((HID, TOK), BF16),
            vmem((WIDE, D), BF16), vmem((WIDE, TOK), BF16), vmem((TOK, WIDE), BF16), vmem((16, TOK, COLS), BF16),
            vmem((CHUNKS, 2, WIDE, COLS), F32), vmem((CHUNKS, 2, 2, XR, COLS), BF16),
            vmem((CHUNKS, 3, 2, XR, COLS), BF16), vmem((CHUNKS, 2, XR, COLS), BF16),
            vmem((CHUNKS, 3, ZR, COLS), BF16), vmem((CHUNKS, 2, XR, COLS), F32),
            vmem((CHUNKS, 3, ZR, COLS), BF16),
            vmem((8, TOK, COLS), F32), vmem((8, TOK, COLS), BF16), vmem((8, TOK, COLS), BF16),
            vmem((2, 2, TOK, COLS), F32), vmem((2, 2, TOK, COLS), BF16), vmem((2, 3, TOK, COLS), BF16),
            vmem((2, TOK, COLS), BF16), vmem((TOK, COLS), BF16),
            dma((6,)), dma((CHUNKS,)), dma((16,)), dma((16,)), dma((CHUNKS, 21)), dma((CHUNKS, 21)), dma((8,)), dma((8,)),
            dma((2, 3)), dma((2, 3)), dma, dma,
        ],
        compiler_params=pltpu.CompilerParams(
            collective_id=0, has_side_effects=True, vmem_limit_bytes=63 * 1024 * 1024
        ),
        cost_estimate=pl.CostEstimate(flops=5 * 10**9, bytes_accessed=10**7, transcendentals=0),
    )(*args)


def finish_kernel(
    w_h, own_h, last_h, x_h, gate_h, up_h, w_v, own_v, last_v, x_v, gate_v, up_v, in_sem, x_sem, out_sem
):
    wide = D // STEPS
    loads = []
    for i in range(STEPS):
        blocks = slice(i * (16 // STEPS), (i + 1) * (16 // STEPS))
        loads.append(pltpu.make_async_copy(w_h.at[blocks], w_v.at[blocks], in_sem.at[i]))
    loads.append(pltpu.make_async_copy(own_h, own_v, x_sem.at[0]))
    loads.append(pltpu.make_async_copy(last_h, last_v, x_sem.at[1]))
    for load in loads:
        load.start()
    stores = []
    for i in range(STEPS):
        loads[i].wait()
        for b in range(i * (16 // STEPS), (i + 1) * (16 // STEPS)):
            cols = slice(b * COLS, (b + 1) * COLS)
            gate_v[:, cols] = w_v[b, 0:HID, :].astype(F32)
            up_v[:, cols] = w_v[b, HID:WIDE, :].astype(F32)
        cols = slice(i * wide, (i + 1) * wide)
        stores.append(pltpu.make_async_copy(gate_v.at[:, cols], gate_h.at[:, cols], out_sem.at[2 * i]))
        stores.append(pltpu.make_async_copy(up_v.at[:, cols], up_h.at[:, cols], out_sem.at[2 * i + 1]))
        stores[-2].start()
        stores[-1].start()
    loads[-2].wait()
    loads[-1].wait()
    x_v[...] = own_v[...] + last_v[...].astype(F32)
    stores.append(pltpu.make_async_copy(x_v, x_h, x_sem.at[2]))
    stores[-1].start()
    for store in stores:
        store.wait()


def finish(w, own, last):
    vmem = pltpu.VMEM
    return pl.pallas_call(
        finish_kernel,
        name="finish",
        out_shape=(
            jax.ShapeDtypeStruct((TOK, COLS), F32),
            jax.ShapeDtypeStruct((HID, D), F32),
            jax.ShapeDtypeStruct((HID, D), F32),
        ),
        in_specs=[pl.BlockSpec(memory_space=pl.ANY)] * 3,
        out_specs=[pl.BlockSpec(memory_space=pl.ANY)] * 3,
        scratch_shapes=[
            vmem((16, WIDE, COLS), BF16), vmem((TOK, COLS), F32), vmem((TOK, COLS), BF16), vmem((TOK, COLS), F32),
            vmem((HID, D), F32), vmem((HID, D), F32),
            pltpu.SemaphoreType.DMA((STEPS,)), pltpu.SemaphoreType.DMA((3,)), pltpu.SemaphoreType.DMA((2 * STEPS,)),
        ],
        compiler_params=pltpu.CompilerParams(vmem_limit_bytes=63 * 1024 * 1024),
        cost_estimate=pl.CostEstimate(flops=10**7, bytes_accessed=10**7, transcendentals=0),
    )(w, own, last)


def body(activations, *others):
    input_grad, gate_t, up_t = finish(*exchange(activations, *(a.T for a in others)))
    return input_grad, gate_t.T, up_t.T


def solution(mesh):
    spread = ("row", "col")
    in_specs = (P("dp", spread),) * 4 + (P(None, spread),) * 2
    out_specs = (P("dp", spread), P(None, spread), P(None, spread))
    return jax.shard_map(body, mesh=mesh, in_specs=in_specs, out_specs=out_specs, check_vma=False)
```

```python
import functools

import jax
import jax.numpy as jnp
from jax import lax
from jax.experimental import pallas as pl
from jax.experimental.pallas import tpu as pltpu
from jax.sharding import PartitionSpec as P

ROOT_TWO_PI = 0.7978845608028654
CUBIC = 0.044715
MESH = pl.DeviceIdType.MESH
F32, BF16 = jnp.float32, jnp.bfloat16

TOK = 1024
HID = 320
WIDE = 2 * HID
COLS = 128
D = 2048
STEPS = 8
CHUNKS = 8
XR = WIDE // 4
ZR = XR // 2


ORDER = (
    ("c0", 0), ("flip",), ("c1", 0), ("ag_nearp", 0), ("ag_pair",), ("b0", 3), ("ag_nearm", 0), ("b0", 1), ("c0", 2),
    ("b0", 0), ("c2", 0), ("c0", 3), ("c0", 1), ("b0", 5), ("b0", 2), ("c1", 2), ("c1", 3), ("c4", 0),
    ("ag_nearm", 1), ("c1", 1), ("ag_nearp", 1), ("c0", 5), ("c2", 2), ("b0", 7), ("c2", 3), ("c0", 4), ("zin", 0, 2),
    ("ag_far", 0), ("b1", 0), ("c2", 1), ("b0", 6), ("c1", 5), ("ag_far", 1), ("b0", 4), ("c0", 6), ("c4", 2),
    ("zin", 0, 1), ("c0", 7), ("c1", 4), ("c2", 5), ("b1", 1), ("zin", 0, 3), ("c4", 1), ("c4", 3), ("c1", 7),
    ("c1", 6), ("zin", 2, 1), ("c8", 0, 0), ("c4", 5), ("c2", 4), ("zin", 3, 1), ("zin", 3, 2), ("zin", 3, 3),
    ("c2", 7), ("zin", 2, 3), ("zin", 5, 2), ("b2", 1), ("c8", 0, 1), ("zin", 5, 3), ("c2", 6), ("zin", 1, 1),
    ("zin", 5, 1), ("c8", 0, 3), ("c8", 3, 1), ("zin", 2, 2), ("c4", 4), ("c8", 2, 1), ("zin", 1, 3), ("c8", 3, 3),
    ("b2", 0), ("c8", 3, 2), ("c4", 7), ("c8", 5, 3), ("c8", 1, 0), ("c8", 3, 0), ("c8", 5, 2), ("zin", 1, 2),
    ("c4", 6), ("c8", 0, 2), ("c8", 2, 2), ("zin", 4, 2), ("c8", 2, 3), ("c8", 7, 0), ("c8", 5, 0), ("zin", 4, 1),
    ("c8", 4, 0), ("zin", 7, 2), ("zin", 4, 3), ("b3",), ("c8", 1, 1), ("zin", 7, 3), ("zin", 7, 1), ("c9", 3),
    ("zin", 6, 2), ("zin", 6, 1), ("c8", 5, 1), ("zin", 6, 3), ("c8", 1, 3), ("c8", 4, 1), ("c8", 6, 0), ("c8", 4, 2),
    ("c8", 7, 2), ("c8", 2, 0), ("c9", 0), ("c8", 7, 3), ("c8", 1, 2), ("c8", 6, 2), ("c8", 4, 3), ("c8", 6, 1),
    ("c8", 7, 1), ("c8", 6, 3), ("b4",), ("c9", 5), ("c9", 2), ("c9", 4), ("c9", 7), ("c9", 1), ("c9", 6),
)


def geglu_grads(gate_input, up_input, hidden_grad):
    gate_pre = gate_input.astype(F32)
    up_pre = up_input.astype(F32)
    grad_hidden = hidden_grad.astype(F32)
    tanh_part = jnp.tanh(ROOT_TWO_PI * (gate_pre + CUBIC * gate_pre * gate_pre * gate_pre))
    gelu_value = 0.5 * gate_pre * (1.0 + tanh_part)
    gelu_slope = 0.5 * (1.0 + tanh_part) + 0.5 * gate_pre * (
        1.0 - tanh_part * tanh_part
    ) * ROOT_TWO_PI * (1.0 + 3.0 * CUBIC * gate_pre * gate_pre)
    return (grad_hidden * up_pre * gelu_slope).astype(BF16), (grad_hidden * gelu_value).astype(BF16)


def kernel(
    act_h, gate_h, up_h, hid_h, wg_h, wu_h,
    w_hbm, own_out, last_out,
    w_out,
    gate_v, up_v, hid_v, wp, gp_t, gp, ag,
    part, xs, xr, x3, qs, q1, zr,
    pkeep, bs, br, ykeep, ys, yr, y3, tz,
    in_sem, out_sem, ag_recv, ag_send, c_recv, c_send, b_recv, b_send, y_recv, y_send, t_recv, t_send,
):
    dp, row, col = lax.axis_index("dp"), lax.axis_index("row"), lax.axis_index("col")
    zh, x = dp // 4, lax.rem(dp, 4)
    y, core = col // 2, lax.rem(col, 2)
    s = 2 * core - 1

    def at(base, step):
        return lax.rem(base + step + 4, 4)

    def dev(dx=0, dzh=0, dy=0, flip_row=False, flip_core=False):
        return (
            at(zh, dzh) * 4 + at(x, dx),
            1 - row if flip_row else row,
            at(y, dy) * 2 + (1 - core if flip_core else core),
        )

    x_up, x_down = dev(dx=s), dev(dx=-s)
    z_up, z_down = dev(dzh=s), dev(dzh=-s)
    y_up, y_down = dev(dy=s), dev(dy=-s)
    z_far = dev(dzh=2)
    pair, mate = dev(flip_row=True), dev(flip_core=True)

    def place(other_row, dy, other_core=False):
        return (1 - row if other_row else row) * 8 + at(y, dy) * 2 + (1 - core if other_core else core)

    own = place(False, 0)
    loads = []
    for n, (src, dst) in enumerate(
        (
            (act_h, ag.at[own]), (gate_h, gate_v), (up_h, up_v), (hid_h, hid_v),
            (wg_h, wp.at[0:HID]), (wu_h, wp.at[HID:WIDE]),
        )
    ):
        loads.append(pltpu.make_async_copy(src, dst, in_sem.at[n]))
        loads[-1].start()

    barrier = pltpu.get_barrier_semaphore()
    for other in (x_up, x_down, z_up, z_down, z_far, y_up, y_down, pair, mate):
        pl.semaphore_signal(barrier, inc=1, device_id=other, device_id_type=MESH)

    sent = []

    def send(src, dst, send_sem, recv_sem, to):
        copy = pltpu.make_async_remote_copy(
            src_ref=src, dst_ref=dst, send_sem=send_sem, recv_sem=recv_sem,
            device_id=to, device_id_type=MESH,
        )
        copy.start()
        sent.append(copy)

    def arrived(dst, recv_sem, send_sem):
        pltpu.make_async_remote_copy(
            src_ref=dst, dst_ref=dst, send_sem=send_sem, recv_sem=recv_sem,
            device_id=mate, device_id_type=MESH,
        ).wait_recv()

    n_ag = [0]

    def ag_give(slot, to):
        send(ag.at[slot], ag.at[slot], ag_send.at[n_ag[0]], ag_recv.at[slot], to)
        n_ag[0] += 1

    def ag_take(slot):
        arrived(ag.at[slot], ag_recv.at[slot], ag_send.at[0])

    for load in loads[1:4]:
        load.wait()

    def gate_rows(i, carry):
        rows = pl.ds(pl.multiple_of(i * 16, 16), 16)
        gate_grad, up_grad = geglu_grads(gate_v[rows, :], up_v[rows, :], hid_v[rows, :])
        gp_t[rows, :] = gate_grad
        gp_t[pl.ds(pl.multiple_of(HID + i * 16, 16), 16), :] = up_grad
        return carry

    lax.fori_loop(0, HID // 32, gate_rows, 0)

    loads[0].wait()
    pl.semaphore_wait(barrier, 9)
    for to in (pair, y_up, y_down, mate):
        ag_give(own, to)

    lax.fori_loop(HID // 32, HID // 16, gate_rows, 0)

    order = ((False, 0), (True, 0), (False, -s), (False, s), (True, -s), (True, s), (False, 2), (True, 2))

    def first_block(k):
        other_row, dy = order[k]
        return (1 - row if other_row else row) * 8 + at(y, dy) * 2

    def c_give(k, n, src, dst, to):
        send(src, dst, c_send.at[k, n], c_recv.at[k, n], to)

    def c_take(k, n, dst):
        arrived(dst, c_recv.at[k, n], c_send.at[k, n])

    def x_rows(place_x):
        return pl.ds(pl.multiple_of(place_x * XR, XR), XR)

    def c0(k):
        other_row, dy = order[k]
        ag_take(place(other_row, dy, True))
        first = first_block(k)
        both = jnp.concatenate([ag[first], ag[first + 1]], axis=1)
        sums = jnp.dot(gp_t[...], both, preferred_element_type=F32)
        part[k, 0] = sums[:, 0:COLS]
        part[k, 1] = sums[:, COLS : 2 * COLS]
        xs[k, 0] = part[k, :, x_rows(at(x, 2)), :].astype(BF16)
        c_give(k, 0, xs.at[k, 0], xr.at[k, 0], x_up)
        xs[k, 1] = part[k, :, x_rows(at(x, -s)), :].astype(BF16)
        c_give(k, 1, xs.at[k, 1], xr.at[k, 1], x_down)

    def c1(k):
        c_take(k, 0, xr.at[k, 0])
        x3[k] = (part[k, :, x_rows(at(x, s)), :] + xr[k, 0].astype(F32)).astype(BF16)
        c_give(k, 2, x3.at[k], xr.at[k, 2], x_up)

    def c2(k):
        c_take(k, 1, xr.at[k, 1])
        c_take(k, 2, xr.at[k, 2])
        q1[k] = part[k, :, x_rows(x), :] + xr[k, 1].astype(F32) + xr[k, 2].astype(F32)
        for n, (step, to) in enumerate(((2, z_far), (-s, z_down), (s, z_up))):
            qs[k, n] = z_part(k, at(zh, step)).astype(BF16)
            c_give(k, 3 + n, qs.at[k, n], zr.at[k, n], to)

    def z_part(k, place_z):
        return q1[k, place_z // 2, pl.ds(pl.multiple_of(lax.rem(place_z, 2) * ZR, ZR), ZR), :]

    def out_part(k, place_x, place_z):
        rows = pl.ds(pl.multiple_of(place_x * XR + lax.rem(place_z, 2) * ZR, ZR), ZR)
        return w_out.at[first_block(k) + place_z // 2, rows, :]

    z_from = (0, -s, s, 2)

    def c4(k):
        for n in range(3):
            c_take(k, 3 + n, zr.at[k, n])
        total = z_part(k, zh) + zr[k, 0].astype(F32) + zr[k, 1].astype(F32) + zr[k, 2].astype(F32)
        mine = out_part(k, x, zh)
        mine[...] = total.astype(BF16)
        for n, to in enumerate((z_up, z_down, z_far)):
            c_give(k, 6 + n, mine, mine, to)
        along_x(k, 0)

    def along_x(k, j):
        held = out_part(k, x, at(zh, z_from[j]))
        c_give(k, 9 + j, held, held, x_up)
        c_give(k, 13 + j, held, held, x_down)

    def z_part_in(k, j):
        c_take(k, 5 + j, out_part(k, x, at(zh, z_from[j])))
        along_x(k, j)

    def c8(k, j):
        got = out_part(k, at(x, -s), at(zh, z_from[j]))
        c_take(k, 9 + j, got)
        c_give(k, 17 + j, got, got, x_up)

    def save(k):
        pair_of = pl.ds(first_block(k), 2)
        return pltpu.make_async_copy(w_out.at[pair_of], w_hbm.at[pair_of], out_sem.at[k])

    def c9(k):
        for j in range(4):
            c_take(k, 13 + j, out_part(k, at(x, s), at(zh, z_from[j])))
            c_take(k, 17 + j, out_part(k, at(x, 2), at(zh, z_from[j])))
        save(k).start()

    def ag_pair():
        slot = place(True, 0)
        ag_take(slot)
        for to in (y_up, y_down, mate):
            ag_give(slot, to)

    def ag_nearm(other_row):
        slot = place(other_row, -s)
        ag_take(slot)
        ag_give(slot, y_up)
        ag_give(slot, mate)

    def ag_nearp(other_row):
        slot = place(other_row, s)
        ag_take(slot)
        ag_give(slot, mate)

    def ag_far(other_row):
        slot = place(other_row, 2)
        ag_take(slot)
        ag_give(slot, mate)

    def flip():
        loads[4].wait()
        loads[5].wait()
        for i in range(TOK // 128):
            rows = slice(i * 128, i * 128 + 128)
            gp[rows, :] = gp_t[:, rows].T

    def b0(i):
        first = ((i // 4) * 8 + at(y, i % 4) * 2) * COLS
        mine = wp[:, pl.ds(pl.multiple_of(first + core * COLS, COLS), COLS)]
        others = wp[:, pl.ds(pl.multiple_of(first + (1 - core) * COLS, COLS), COLS)]
        both = jnp.concatenate([mine, others], axis=1)

        def step(r, carry):
            rows = pl.ds(pl.multiple_of(r * 256, 256), 256)
            sums = jnp.dot(gp[rows, :], both, preferred_element_type=F32)
            pkeep[i, rows, :] = sums[:, 0:COLS]
            bs[i, rows, :] = sums[:, COLS : 2 * COLS].astype(BF16)
            return carry

        lax.fori_loop(0, TOK // 256, step, 0)
        send(bs.at[i], br.at[i], b_send.at[i], b_recv.at[i], mate)

    def b1(r):
        for i in range(4 * r, 4 * r + 4):
            arrived(br.at[i], b_recv.at[i], b_send.at[i])

        def pair_sum(off):
            i = 4 * r + at(0, off)
            return pkeep[i] + br[i].astype(F32)

        ys[r, 0] = pair_sum(2).astype(BF16)
        send(ys.at[r, 0], yr.at[r, 0], y_send.at[r, 0], y_recv.at[r, 0], y_up)
        ys[r, 1] = pair_sum(-s).astype(BF16)
        send(ys.at[r, 1], yr.at[r, 1], y_send.at[r, 1], y_recv.at[r, 1], y_down)
        ykeep[r, 0] = pair_sum(s)
        ykeep[r, 1] = pair_sum(0)

    def b2(r):
        arrived(yr.at[r, 0], y_recv.at[r, 0], y_send.at[r, 0])
        y3[r] = (ykeep[r, 0] + yr[r, 0].astype(F32)).astype(BF16)
        send(y3.at[r], yr.at[r, 2], y_send.at[r, 2], y_recv.at[r, 2], y_up)

    def b3():
        for r in range(2):
            for n in (1, 2):
                arrived(yr.at[r, n], y_recv.at[r, n], y_send.at[r, n])

        def total(r):
            return ykeep[r, 1] + yr[r, 1].astype(F32) + yr[r, 2].astype(F32)

        tz[...] = total(1 - row).astype(BF16)
        send(tz, last_out, t_send, t_recv, pair)
        own_out[...] = total(row)

    def b4():
        arrived(last_out, t_recv, t_send)

    steps = dict(
        c0=c0, c1=c1, c2=c2, c4=c4, zin=z_part_in, c8=c8, c9=c9, flip=flip, b0=b0, b1=b1, b2=b2, b3=b3, b4=b4,
        ag_pair=ag_pair, ag_nearm=ag_nearm, ag_nearp=ag_nearp, ag_far=ag_far,
    )
    for name, *n in ORDER:
        steps[name](*n)
    for copy in sent:
        copy.wait_send()
    for k in range(CHUNKS):
        save(k).wait()


def exchange(*args):
    vmem = pltpu.VMEM
    dma = pltpu.SemaphoreType.DMA
    return pl.pallas_call(
        kernel,
        name="exchange",
        out_shape=(
            jax.ShapeDtypeStruct((16, WIDE, COLS), BF16),
            jax.ShapeDtypeStruct((TOK, COLS), F32),
            jax.ShapeDtypeStruct((TOK, COLS), BF16),
        ),
        in_specs=[pl.BlockSpec(memory_space=pl.ANY)] * 6,
        out_specs=[pl.BlockSpec(memory_space=pl.ANY)] + [pl.BlockSpec(memory_space=pltpu.VMEM)] * 2,
        scratch_shapes=[
            vmem((16, WIDE, COLS), BF16),
            vmem((HID, TOK), BF16), vmem((HID, TOK), BF16), vmem((HID, TOK), BF16),
            vmem((WIDE, D), BF16), vmem((WIDE, TOK), BF16), vmem((TOK, WIDE), BF16), vmem((16, TOK, COLS), BF16),
            vmem((CHUNKS, 2, WIDE, COLS), F32), vmem((CHUNKS, 2, 2, XR, COLS), BF16),
            vmem((CHUNKS, 3, 2, XR, COLS), BF16), vmem((CHUNKS, 2, XR, COLS), BF16),
            vmem((CHUNKS, 3, ZR, COLS), BF16), vmem((CHUNKS, 2, XR, COLS), F32),
            vmem((CHUNKS, 3, ZR, COLS), BF16),
            vmem((8, TOK, COLS), F32), vmem((8, TOK, COLS), BF16), vmem((8, TOK, COLS), BF16),
            vmem((2, 2, TOK, COLS), F32), vmem((2, 2, TOK, COLS), BF16), vmem((2, 3, TOK, COLS), BF16),
            vmem((2, TOK, COLS), BF16), vmem((TOK, COLS), BF16),
            dma((6,)), dma((CHUNKS,)), dma((16,)), dma((16,)), dma((CHUNKS, 21)), dma((CHUNKS, 21)), dma((8,)), dma((8,)),
            dma((2, 3)), dma((2, 3)), dma, dma,
        ],
        compiler_params=pltpu.CompilerParams(
            collective_id=0, has_side_effects=True, vmem_limit_bytes=63 * 1024 * 1024
        ),
        cost_estimate=pl.CostEstimate(flops=5 * 10**9, bytes_accessed=10**7, transcendentals=0),
    )(*args)


def finish_kernel(
    w_h, own_h, last_h, x_h, gate_h, up_h, w_v, own_v, last_v, x_v, gate_v, up_v, in_sem, x_sem, out_sem
):
    wide = D // STEPS
    loads = []
    for i in range(STEPS):
        blocks = slice(i * (16 // STEPS), (i + 1) * (16 // STEPS))
        loads.append(pltpu.make_async_copy(w_h.at[blocks], w_v.at[blocks], in_sem.at[i]))
    loads.append(pltpu.make_async_copy(own_h, own_v, x_sem.at[0]))
    loads.append(pltpu.make_async_copy(last_h, last_v, x_sem.at[1]))
    for load in loads:
        load.start()
    stores = []
    for i in range(STEPS):
        loads[i].wait()
        for b in range(i * (16 // STEPS), (i + 1) * (16 // STEPS)):
            cols = slice(b * COLS, (b + 1) * COLS)
            gate_v[:, cols] = w_v[b, 0:HID, :].astype(F32)
            up_v[:, cols] = w_v[b, HID:WIDE, :].astype(F32)
        cols = slice(i * wide, (i + 1) * wide)
        stores.append(pltpu.make_async_copy(gate_v.at[:, cols], gate_h.at[:, cols], out_sem.at[2 * i]))
        stores.append(pltpu.make_async_copy(up_v.at[:, cols], up_h.at[:, cols], out_sem.at[2 * i + 1]))
        stores[-2].start()
        stores[-1].start()
    loads[-2].wait()
    loads[-1].wait()
    x_v[...] = own_v[...] + last_v[...].astype(F32)
    stores.append(pltpu.make_async_copy(x_v, x_h, x_sem.at[2]))
    stores[-1].start()
    for store in stores:
        store.wait()


def finish(w, own, last):
    vmem = pltpu.VMEM
    return pl.pallas_call(
        finish_kernel,
        name="finish",
        out_shape=(
            jax.ShapeDtypeStruct((TOK, COLS), F32),
            jax.ShapeDtypeStruct((HID, D), F32),
            jax.ShapeDtypeStruct((HID, D), F32),
        ),
        in_specs=[pl.BlockSpec(memory_space=pl.ANY)] * 3,
        out_specs=[pl.BlockSpec(memory_space=pl.ANY)] * 3,
        scratch_shapes=[
            vmem((16, WIDE, COLS), BF16), vmem((TOK, COLS), F32), vmem((TOK, COLS), BF16), vmem((TOK, COLS), F32),
            vmem((HID, D), F32), vmem((HID, D), F32),
            pltpu.SemaphoreType.DMA((STEPS,)), pltpu.SemaphoreType.DMA((3,)), pltpu.SemaphoreType.DMA((2 * STEPS,)),
        ],
        compiler_params=pltpu.CompilerParams(vmem_limit_bytes=63 * 1024 * 1024),
        cost_estimate=pl.CostEstimate(flops=10**7, bytes_accessed=10**7, transcendentals=0),
    )(w, own, last)


def body(activations, *others):
    input_grad, gate_t, up_t = finish(*exchange(activations, *(a.T for a in others)))
    return input_grad, gate_t.T, up_t.T


def solution(mesh):
    spread = ("row", "col")
    in_specs = (P("dp", spread),) * 4 + (P(None, spread),) * 2
    out_specs = (P("dp", spread), P(None, spread), P(None, spread))
    return jax.shard_map(body, mesh=mesh, in_specs=in_specs, out_specs=out_specs, check_vma=False)
```

```python
import functools

import jax
import jax.numpy as jnp
from jax import lax
from jax.experimental import pallas as pl
from jax.experimental.pallas import tpu as pltpu
from jax.sharding import PartitionSpec as P

ROOT_TWO_PI = 0.7978845608028654
CUBIC = 0.044715
MESH = pl.DeviceIdType.MESH
F32, BF16 = jnp.float32, jnp.bfloat16

TOK = 1024
HID = 320
WIDE = 2 * HID
COLS = 128
D = 2048
STEPS = 8
CHUNKS = 8
XR = WIDE // 4
ZR = XR // 2


ORDER = (
    ("c0", 0), ("flip",), ("c1", 0), ("ag_nearp", 0), ("ag_pair",), ("b0", 3), ("ag_nearm", 0), ("b0", 1), ("c0", 2),
    ("b0", 0), ("c2", 0), ("c0", 3), ("c0", 1), ("b0", 5), ("b0", 2), ("c1", 2), ("c1", 3), ("c4", 0),
    ("ag_nearm", 1), ("c1", 1), ("ag_nearp", 1), ("c0", 5), ("c2", 2), ("b0", 7), ("c2", 3), ("c0", 4), ("zin", 0, 2),
    ("ag_far", 0), ("b1", 0), ("c2", 1), ("b0", 6), ("c1", 5), ("ag_far", 1), ("b0", 4), ("c0", 6), ("c4", 2),
    ("zin", 0, 1), ("c0", 7), ("c1", 4), ("c2", 5), ("b1", 1), ("zin", 0, 3), ("c4", 1), ("c4", 3), ("c1", 7),
    ("c1", 6), ("zin", 2, 1), ("c8", 0, 0), ("c4", 5), ("c2", 4), ("zin", 3, 1), ("zin", 3, 2), ("zin", 3, 3),
    ("c2", 7), ("zin", 2, 3), ("zin", 5, 2), ("b2", 1), ("c8", 0, 1), ("zin", 5, 3), ("c2", 6), ("zin", 1, 1),
    ("zin", 5, 1), ("c8", 0, 3), ("c8", 3, 1), ("zin", 2, 2), ("c4", 4), ("c8", 2, 1), ("zin", 1, 3), ("c8", 3, 3),
    ("b2", 0), ("c8", 3, 2), ("c4", 7), ("c8", 5, 3), ("c8", 1, 0), ("c8", 3, 0), ("c8", 5, 2), ("zin", 1, 2),
    ("c4", 6), ("c8", 0, 2), ("c8", 2, 2), ("zin", 4, 2), ("c8", 2, 3), ("c8", 7, 0), ("c8", 5, 0), ("zin", 4, 1),
    ("c8", 4, 0), ("zin", 7, 2), ("zin", 4, 3), ("b3",), ("c8", 1, 1), ("zin", 7, 3), ("zin", 7, 1), ("c9", 3),
    ("zin", 6, 2), ("zin", 6, 1), ("c8", 5, 1), ("zin", 6, 3), ("c8", 1, 3), ("c8", 4, 1), ("c8", 6, 0), ("c8", 4, 2),
    ("c8", 7, 2), ("c8", 2, 0), ("c9", 0), ("c8", 7, 3), ("c8", 1, 2), ("c8", 6, 2), ("c8", 4, 3), ("c8", 6, 1),
    ("c8", 7, 1), ("c8", 6, 3), ("b4",), ("c9", 5), ("c9", 2), ("c9", 4), ("c9", 7), ("c9", 1), ("c9", 6),
)


def geglu_grads(gate_input, up_input, hidden_grad):
    gate_pre = gate_input.astype(F32)
    up_pre = up_input.astype(F32)
    grad_hidden = hidden_grad.astype(F32)
    tanh_part = jnp.tanh(ROOT_TWO_PI * (gate_pre + CUBIC * gate_pre * gate_pre * gate_pre))
    gelu_value = 0.5 * gate_pre * (1.0 + tanh_part)
    gelu_slope = 0.5 * (1.0 + tanh_part) + 0.5 * gate_pre * (
        1.0 - tanh_part * tanh_part
    ) * ROOT_TWO_PI * (1.0 + 3.0 * CUBIC * gate_pre * gate_pre)
    return (grad_hidden * up_pre * gelu_slope).astype(BF16), (grad_hidden * gelu_value).astype(BF16)


def kernel(
    act_h, gate_h, up_h, hid_h, wg_h, wu_h,
    w_hbm, own_out, last_out,
    w_out,
    gate_v, up_v, hid_v, wp, gp_t, gp, ag,
    part, xs, xr, x3, qs, q1, zr,
    pkeep, bs, br, ykeep, ys, yr, y3, tz,
    in_sem, out_sem, ag_recv, ag_send, c_recv, c_send, b_recv, b_send, y_recv, y_send, t_recv, t_send,
):
    dp, row, col = lax.axis_index("dp"), lax.axis_index("row"), lax.axis_index("col")
    zh, x = dp // 4, lax.rem(dp, 4)
    y, core = col // 2, lax.rem(col, 2)
    s = 2 * core - 1

    def at(base, step):
        return lax.rem(base + step + 4, 4)

    def dev(dx=0, dzh=0, dy=0, flip_row=False, flip_core=False):
        return (
            at(zh, dzh) * 4 + at(x, dx),
            1 - row if flip_row else row,
            at(y, dy) * 2 + (1 - core if flip_core else core),
        )

    x_up, x_down = dev(dx=s), dev(dx=-s)
    z_up, z_down = dev(dzh=s), dev(dzh=-s)
    y_up, y_down = dev(dy=s), dev(dy=-s)
    z_far = dev(dzh=2)
    pair, mate = dev(flip_row=True), dev(flip_core=True)

    def place(other_row, dy, other_core=False):
        return (1 - row if other_row else row) * 8 + at(y, dy) * 2 + (1 - core if other_core else core)

    own = place(False, 0)
    loads = []
    for n, (src, dst) in enumerate(
        (
            (act_h, ag.at[own]), (gate_h, gate_v), (up_h, up_v), (hid_h, hid_v),
            (wg_h, wp.at[0:HID]), (wu_h, wp.at[HID:WIDE]),
        )
    ):
        loads.append(pltpu.make_async_copy(src, dst, in_sem.at[n]))
        if n < 4:
            loads[-1].start()

    barrier = pltpu.get_barrier_semaphore()
    for other in (x_up, x_down, z_up, z_down, z_far, y_up, y_down, pair, mate):
        pl.semaphore_signal(barrier, inc=1, device_id=other, device_id_type=MESH)

    sent = []

    def send(src, dst, send_sem, recv_sem, to):
        copy = pltpu.make_async_remote_copy(
            src_ref=src, dst_ref=dst, send_sem=send_sem, recv_sem=recv_sem,
            device_id=to, device_id_type=MESH,
        )
        copy.start()
        sent.append(copy)

    def arrived(dst, recv_sem, send_sem):
        pltpu.make_async_remote_copy(
            src_ref=dst, dst_ref=dst, send_sem=send_sem, recv_sem=recv_sem,
            device_id=mate, device_id_type=MESH,
        ).wait_recv()

    n_ag = [0]

    def ag_give(slot, to):
        send(ag.at[slot], ag.at[slot], ag_send.at[n_ag[0]], ag_recv.at[slot], to)
        n_ag[0] += 1

    def ag_take(slot):
        arrived(ag.at[slot], ag_recv.at[slot], ag_send.at[0])

    for load in loads[1:4]:
        load.wait()

    def gate_rows(i, carry):
        rows = pl.ds(pl.multiple_of(i * 16, 16), 16)
        gate_grad, up_grad = geglu_grads(gate_v[rows, :], up_v[rows, :], hid_v[rows, :])
        gp_t[rows, :] = gate_grad
        gp_t[pl.ds(pl.multiple_of(HID + i * 16, 16), 16), :] = up_grad
        return carry

    lax.fori_loop(0, HID // 32, gate_rows, 0)

    loads[0].wait()
    pl.semaphore_wait(barrier, 9)
    for to in (pair, y_up, y_down, mate):
        ag_give(own, to)
    for load in loads[4:]:
        load.start()

    lax.fori_loop(HID // 32, HID // 16, gate_rows, 0)

    order = ((False, 0), (True, 0), (False, -s), (False, s), (True, -s), (True, s), (False, 2), (True, 2))

    def first_block(k):
        other_row, dy = order[k]
        return (1 - row if other_row else row) * 8 + at(y, dy) * 2

    def c_give(k, n, src, dst, to):
        send(src, dst, c_send.at[k, n], c_recv.at[k, n], to)

    def c_take(k, n, dst):
        arrived(dst, c_recv.at[k, n], c_send.at[k, n])

    def x_rows(place_x):
        return pl.ds(pl.multiple_of(place_x * XR, XR), XR)

    def c0(k):
        other_row, dy = order[k]
        ag_take(place(other_row, dy, True))
        first = first_block(k)
        both = jnp.concatenate([ag[first], ag[first + 1]], axis=1)
        sums = jnp.dot(gp_t[...], both, preferred_element_type=F32)
        part[k, 0] = sums[:, 0:COLS]
        part[k, 1] = sums[:, COLS : 2 * COLS]
        xs[k, 0] = part[k, :, x_rows(at(x, 2)), :].astype(BF16)
        c_give(k, 0, xs.at[k, 0], xr.at[k, 0], x_up)
        xs[k, 1] = part[k, :, x_rows(at(x, -s)), :].astype(BF16)
        c_give(k, 1, xs.at[k, 1], xr.at[k, 1], x_down)

    def c1(k):
        c_take(k, 0, xr.at[k, 0])
        x3[k] = (part[k, :, x_rows(at(x, s)), :] + xr[k, 0].astype(F32)).astype(BF16)
        c_give(k, 2, x3.at[k], xr.at[k, 2], x_up)

    def c2(k):
        c_take(k, 1, xr.at[k, 1])
        c_take(k, 2, xr.at[k, 2])
        q1[k] = part[k, :, x_rows(x), :] + xr[k, 1].astype(F32) + xr[k, 2].astype(F32)
        for n, (step, to) in enumerate(((2, z_far), (-s, z_down), (s, z_up))):
            qs[k, n] = z_part(k, at(zh, step)).astype(BF16)
            c_give(k, 3 + n, qs.at[k, n], zr.at[k, n], to)

    def z_part(k, place_z):
        return q1[k, place_z // 2, pl.ds(pl.multiple_of(lax.rem(place_z, 2) * ZR, ZR), ZR), :]

    def out_part(k, place_x, place_z):
        rows = pl.ds(pl.multiple_of(place_x * XR + lax.rem(place_z, 2) * ZR, ZR), ZR)
        return w_out.at[first_block(k) + place_z // 2, rows, :]

    z_from = (0, -s, s, 2)

    def c4(k):
        for n in range(3):
            c_take(k, 3 + n, zr.at[k, n])
        total = z_part(k, zh) + zr[k, 0].astype(F32) + zr[k, 1].astype(F32) + zr[k, 2].astype(F32)
        mine = out_part(k, x, zh)
        mine[...] = total.astype(BF16)
        for n, to in enumerate((z_up, z_down, z_far)):
            c_give(k, 6 + n, mine, mine, to)
        along_x(k, 0)

    def along_x(k, j):
        held = out_part(k, x, at(zh, z_from[j]))
        c_give(k, 9 + j, held, held, x_up)
        c_give(k, 13 + j, held, held, x_down)

    def z_part_in(k, j):
        c_take(k, 5 + j, out_part(k, x, at(zh, z_from[j])))
        along_x(k, j)

    def c8(k, j):
        got = out_part(k, at(x, -s), at(zh, z_from[j]))
        c_take(k, 9 + j, got)
        c_give(k, 17 + j, got, got, x_up)

    def save(k):
        pair_of = pl.ds(first_block(k), 2)
        return pltpu.make_async_copy(w_out.at[pair_of], w_hbm.at[pair_of], out_sem.at[k])

    def c9(k):
        for j in range(4):
            c_take(k, 13 + j, out_part(k, at(x, s), at(zh, z_from[j])))
            c_take(k, 17 + j, out_part(k, at(x, 2), at(zh, z_from[j])))
        save(k).start()

    def ag_pair():
        slot = place(True, 0)
        ag_take(slot)
        for to in (y_up, y_down, mate):
            ag_give(slot, to)

    def ag_nearm(other_row):
        slot = place(other_row, -s)
        ag_take(slot)
        ag_give(slot, y_up)
        ag_give(slot, mate)

    def ag_nearp(other_row):
        slot = place(other_row, s)
        ag_take(slot)
        ag_give(slot, mate)

    def ag_far(other_row):
        slot = place(other_row, 2)
        ag_take(slot)
        ag_give(slot, mate)

    def flip():
        loads[4].wait()
        loads[5].wait()
        for i in range(TOK // 128):
            rows = slice(i * 128, i * 128 + 128)
            gp[rows, :] = gp_t[:, rows].T

    def b0(i):
        first = ((i // 4) * 8 + at(y, i % 4) * 2) * COLS
        mine = wp[:, pl.ds(pl.multiple_of(first + core * COLS, COLS), COLS)]
        others = wp[:, pl.ds(pl.multiple_of(first + (1 - core) * COLS, COLS), COLS)]
        both = jnp.concatenate([mine, others], axis=1)

        def step(r, carry):
            rows = pl.ds(pl.multiple_of(r * 256, 256), 256)
            sums = jnp.dot(gp[rows, :], both, preferred_element_type=F32)
            pkeep[i, rows, :] = sums[:, 0:COLS]
            bs[i, rows, :] = sums[:, COLS : 2 * COLS].astype(BF16)
            return carry

        lax.fori_loop(0, TOK // 256, step, 0)
        send(bs.at[i], br.at[i], b_send.at[i], b_recv.at[i], mate)

    def b1(r):
        for i in range(4 * r, 4 * r + 4):
            arrived(br.at[i], b_recv.at[i], b_send.at[i])

        def pair_sum(off):
            i = 4 * r + at(0, off)
            return pkeep[i] + br[i].astype(F32)

        ys[r, 0] = pair_sum(2).astype(BF16)
        send(ys.at[r, 0], yr.at[r, 0], y_send.at[r, 0], y_recv.at[r, 0], y_up)
        ys[r, 1] = pair_sum(-s).astype(BF16)
        send(ys.at[r, 1], yr.at[r, 1], y_send.at[r, 1], y_recv.at[r, 1], y_down)
        ykeep[r, 0] = pair_sum(s)
        ykeep[r, 1] = pair_sum(0)

    def b2(r):
        arrived(yr.at[r, 0], y_recv.at[r, 0], y_send.at[r, 0])
        y3[r] = (ykeep[r, 0] + yr[r, 0].astype(F32)).astype(BF16)
        send(y3.at[r], yr.at[r, 2], y_send.at[r, 2], y_recv.at[r, 2], y_up)

    def b3():
        for r in range(2):
            for n in (1, 2):
                arrived(yr.at[r, n], y_recv.at[r, n], y_send.at[r, n])

        def total(r):
            return ykeep[r, 1] + yr[r, 1].astype(F32) + yr[r, 2].astype(F32)

        tz[...] = total(1 - row).astype(BF16)
        send(tz, last_out, t_send, t_recv, pair)
        own_out[...] = total(row)

    def b4():
        arrived(last_out, t_recv, t_send)

    steps = dict(
        c0=c0, c1=c1, c2=c2, c4=c4, zin=z_part_in, c8=c8, c9=c9, flip=flip, b0=b0, b1=b1, b2=b2, b3=b3, b4=b4,
        ag_pair=ag_pair, ag_nearm=ag_nearm, ag_nearp=ag_nearp, ag_far=ag_far,
    )
    for name, *n in ORDER:
        steps[name](*n)
    for copy in sent:
        copy.wait_send()
    for k in range(CHUNKS):
        save(k).wait()


def exchange(*args):
    vmem = pltpu.VMEM
    dma = pltpu.SemaphoreType.DMA
    return pl.pallas_call(
        kernel,
        name="exchange",
        out_shape=(
            jax.ShapeDtypeStruct((16, WIDE, COLS), BF16),
            jax.ShapeDtypeStruct((TOK, COLS), F32),
            jax.ShapeDtypeStruct((TOK, COLS), BF16),
        ),
        in_specs=[pl.BlockSpec(memory_space=pl.ANY)] * 6,
        out_specs=[pl.BlockSpec(memory_space=pl.ANY)] + [pl.BlockSpec(memory_space=pltpu.VMEM)] * 2,
        scratch_shapes=[
            vmem((16, WIDE, COLS), BF16),
            vmem((HID, TOK), BF16), vmem((HID, TOK), BF16), vmem((HID, TOK), BF16),
            vmem((WIDE, D), BF16), vmem((WIDE, TOK), BF16), vmem((TOK, WIDE), BF16), vmem((16, TOK, COLS), BF16),
            vmem((CHUNKS, 2, WIDE, COLS), F32), vmem((CHUNKS, 2, 2, XR, COLS), BF16),
            vmem((CHUNKS, 3, 2, XR, COLS), BF16), vmem((CHUNKS, 2, XR, COLS), BF16),
            vmem((CHUNKS, 3, ZR, COLS), BF16), vmem((CHUNKS, 2, XR, COLS), F32),
            vmem((CHUNKS, 3, ZR, COLS), BF16),
            vmem((8, TOK, COLS), F32), vmem((8, TOK, COLS), BF16), vmem((8, TOK, COLS), BF16),
            vmem((2, 2, TOK, COLS), F32), vmem((2, 2, TOK, COLS), BF16), vmem((2, 3, TOK, COLS), BF16),
            vmem((2, TOK, COLS), BF16), vmem((TOK, COLS), BF16),
            dma((6,)), dma((CHUNKS,)), dma((16,)), dma((16,)), dma((CHUNKS, 21)), dma((CHUNKS, 21)), dma((8,)), dma((8,)),
            dma((2, 3)), dma((2, 3)), dma, dma,
        ],
        compiler_params=pltpu.CompilerParams(
            collective_id=0, has_side_effects=True, vmem_limit_bytes=63 * 1024 * 1024
        ),
        cost_estimate=pl.CostEstimate(flops=5 * 10**9, bytes_accessed=10**7, transcendentals=0),
    )(*args)


def finish_kernel(
    w_h, own_h, last_h, x_h, gate_h, up_h, w_v, own_v, last_v, x_v, gate_v, up_v, in_sem, x_sem, out_sem
):
    wide = D // STEPS
    loads = []
    for i in range(STEPS):
        blocks = slice(i * (16 // STEPS), (i + 1) * (16 // STEPS))
        loads.append(pltpu.make_async_copy(w_h.at[blocks], w_v.at[blocks], in_sem.at[i]))
    loads.append(pltpu.make_async_copy(own_h, own_v, x_sem.at[0]))
    loads.append(pltpu.make_async_copy(last_h, last_v, x_sem.at[1]))
    for load in loads:
        load.start()
    stores = []
    for i in range(STEPS):
        loads[i].wait()
        for b in range(i * (16 // STEPS), (i + 1) * (16 // STEPS)):
            cols = slice(b * COLS, (b + 1) * COLS)
            gate_v[:, cols] = w_v[b, 0:HID, :].astype(F32)
            up_v[:, cols] = w_v[b, HID:WIDE, :].astype(F32)
        cols = slice(i * wide, (i + 1) * wide)
        stores.append(pltpu.make_async_copy(gate_v.at[:, cols], gate_h.at[:, cols], out_sem.at[2 * i]))
        stores.append(pltpu.make_async_copy(up_v.at[:, cols], up_h.at[:, cols], out_sem.at[2 * i + 1]))
        stores[-2].start()
        stores[-1].start()
    loads[-2].wait()
    loads[-1].wait()
    x_v[...] = own_v[...] + last_v[...].astype(F32)
    stores.append(pltpu.make_async_copy(x_v, x_h, x_sem.at[2]))
    stores[-1].start()
    for store in stores:
        store.wait()


def finish(w, own, last):
    vmem = pltpu.VMEM
    return pl.pallas_call(
        finish_kernel,
        name="finish",
        out_shape=(
            jax.ShapeDtypeStruct((TOK, COLS), F32),
            jax.ShapeDtypeStruct((HID, D), F32),
            jax.ShapeDtypeStruct((HID, D), F32),
        ),
        in_specs=[pl.BlockSpec(memory_space=pl.ANY)] * 3,
        out_specs=[pl.BlockSpec(memory_space=pl.ANY)] * 3,
        scratch_shapes=[
            vmem((16, WIDE, COLS), BF16), vmem((TOK, COLS), F32), vmem((TOK, COLS), BF16), vmem((TOK, COLS), F32),
            vmem((HID, D), F32), vmem((HID, D), F32),
            pltpu.SemaphoreType.DMA((STEPS,)), pltpu.SemaphoreType.DMA((3,)), pltpu.SemaphoreType.DMA((2 * STEPS,)),
        ],
        compiler_params=pltpu.CompilerParams(vmem_limit_bytes=63 * 1024 * 1024),
        cost_estimate=pl.CostEstimate(flops=10**7, bytes_accessed=10**7, transcendentals=0),
    )(w, own, last)


def body(activations, *others):
    input_grad, gate_t, up_t = finish(*exchange(activations, *(a.T for a in others)))
    return input_grad, gate_t.T, up_t.T


def solution(mesh):
    spread = ("row", "col")
    in_specs = (P("dp", spread),) * 4 + (P(None, spread),) * 2
    out_specs = (P("dp", spread), P(None, spread), P(None, spread))
    return jax.shard_map(body, mesh=mesh, in_specs=in_specs, out_specs=out_specs, check_vma=False)
```
